128 devices in a mesh: pool: 128 (over z, y, x, core).
Axes of the slice: x: 4, y: 4, z: 4, core: 2. Of those that a mesh axis runs over, the one named last changes fastest.
Arguments:
- queries: bfloat16 [128, 128, 64, 128], P('pool')
- k_new: bfloat16 [128, 128, 8, 128], P('pool')
- v_new: bfloat16 [128, 128, 8, 128], P('pool')
- k_pool: bfloat16 [4096, 16, 8, 128], P('pool')
- v_pool: bfloat16 [4096, 16, 8, 128], P('pool')
- block_table: int32 [128, 64], replicated
- write_ids: int32 [128, 8], P('pool')
Outputs:
- output 1: bfloat16 [128, 128, 64, 128], P('pool')
- output 2: bfloat16 [4096, 16, 8, 128], P('pool')
- output 3: bfloat16 [4096, 16, 8, 128], P('pool')
All inputs are finite; a program needn't handle non-finite values.
Results may differ from the reference program's by a relative error of at most 0.00941793.
Values are sent between devices in bfloat16 or wider.
A program may use at most 1 GiB of HBM per device.

```python
import jax
import jax.numpy as jnp
from jax import lax

NUM_DEVICES = 128
REQ_PER_DEV = 1
CHUNK_LEN = 128
PREFIX_BLOCKS = 64
BLOCKS_PER_DEV = 32
BLOCK_LEN = 16
Q_HEADS = 64
KV_HEADS = 8
HEAD_DIM = 128


def draw_tables(rng_key):
    key_first, key_choice, key_start, key_base, key_write = jax.random.split(rng_key, 5)
    quarter = BLOCKS_PER_DEV // 4
    half_len = PREFIX_BLOCKS // 2
    per_owner = 2 * PREFIX_BLOCKS // NUM_DEVICES
    first_dev = jax.random.randint(key_first, (), 0, NUM_DEVICES)
    dev_choice = jax.random.randint(key_choice, (NUM_DEVICES,), 0, 2)
    win_start = first_dev + jax.random.randint(key_start, (NUM_DEVICES,), 0, NUM_DEVICES // 4)
    row_base = jax.random.randint(key_base, (NUM_DEVICES, REQ_PER_DEV), 0, quarter)
    slot_idx = jnp.arange(half_len)
    pop_owner = (first_dev + slot_idx // per_owner) % NUM_DEVICES
    pop_local = dev_choice[:, None] * per_owner + slot_idx[None, :] % per_owner
    pop_ids = pop_owner[None, :] * BLOCKS_PER_DEV + pop_local
    pop_rows = jnp.broadcast_to(pop_ids[:, None, :], (NUM_DEVICES, REQ_PER_DEV, half_len))
    win_owner = (win_start[:, None] + slot_idx[None, :]) % NUM_DEVICES
    win_local = quarter + (row_base[:, :, None] + slot_idx[None, None, :] // NUM_DEVICES) % quarter
    win_rows = win_owner[:, None, :] * BLOCKS_PER_DEV + win_local
    block_tab = jnp.concatenate([pop_rows, win_rows], axis=-1)
    block_tab = block_tab.reshape(NUM_DEVICES * REQ_PER_DEV, PREFIX_BLOCKS)
    new_blocks = REQ_PER_DEV * CHUNK_LEN // BLOCK_LEN
    write_keys = jax.random.split(key_write, NUM_DEVICES)
    shuffled = jax.vmap(lambda one_key: jax.random.permutation(one_key, BLOCKS_PER_DEV // 2))(write_keys)
    write_tab = shuffled[:, :new_blocks] + BLOCKS_PER_DEV // 2
    write_tab = write_tab.reshape(NUM_DEVICES * REQ_PER_DEV, CHUNK_LEN // BLOCK_LEN)
    return block_tab.astype(jnp.int32), write_tab.astype(jnp.int32)


def setup_inputs(seed: int = 0) -> dict:
    key_q, key_kn, key_vn, key_kp, key_vp, key_tab = jax.random.split(jax.random.key(seed), 6)
    n_rows = NUM_DEVICES * REQ_PER_DEV
    chunk_kv = (n_rows, CHUNK_LEN, KV_HEADS, HEAD_DIM)
    pool_shape = (NUM_DEVICES * BLOCKS_PER_DEV, BLOCK_LEN, KV_HEADS, HEAD_DIM)
    queries = jax.random.normal(key_q, (n_rows, CHUNK_LEN, Q_HEADS, HEAD_DIM), jnp.float32)
    k_new = jax.random.normal(key_kn, chunk_kv, jnp.float32)
    v_new = jax.random.normal(key_vn, chunk_kv, jnp.float32)
    k_pool = jax.random.normal(key_kp, pool_shape, jnp.float32)
    v_pool = jax.random.normal(key_vp, pool_shape, jnp.float32)
    block_table, write_ids = draw_tables(key_tab)
    return {'queries': queries.astype(jnp.bfloat16), 'k_new': k_new.astype(jnp.bfloat16), 'v_new': v_new.astype(jnp.bfloat16), 'k_pool': k_pool.astype(jnp.bfloat16), 'v_pool': v_pool.astype(jnp.bfloat16), 'block_table': block_table, 'write_ids': write_ids}


def attend_one(q_rows, k_all, v_all):
    groups = Q_HEADS // KV_HEADS
    prefix_len = PREFIX_BLOCKS * BLOCK_LEN
    q_grp = q_rows.astype(jnp.float32).reshape(CHUNK_LEN, KV_HEADS, groups, HEAD_DIM)
    scores = jnp.einsum('cgqd,tgd->cgqt', q_grp, k_all.astype(jnp.float32)) * HEAD_DIM ** -0.5
    visible = jnp.arange(prefix_len + CHUNK_LEN)[None, :] <= prefix_len + jnp.arange(CHUNK_LEN)[:, None]
    scores = jnp.where(visible[:, None, None, :], scores, -jnp.inf)
    prob_rows = jax.nn.softmax(scores, axis=-1).astype(jnp.bfloat16).astype(jnp.float32)
    attn_rows = jnp.einsum('cgqt,tgd->cgqd', prob_rows, v_all.astype(jnp.float32))
    return attn_rows.reshape(CHUNK_LEN, Q_HEADS, HEAD_DIM).astype(jnp.bfloat16)


def reference(queries, k_new, v_new, k_pool, v_pool, block_table, write_ids):
    prefix_len = PREFIX_BLOCKS * BLOCK_LEN
    n_rows = NUM_DEVICES * REQ_PER_DEV

    def one_request(row_item):
        q_rows, k_chunk, v_chunk, row_ids = row_item
        k_all = jnp.concatenate([k_pool[row_ids].reshape(prefix_len, KV_HEADS, HEAD_DIM), k_chunk], axis=0)
        v_all = jnp.concatenate([v_pool[row_ids].reshape(prefix_len, KV_HEADS, HEAD_DIM), v_chunk], axis=0)
        return attend_one(q_rows, k_all, v_all)

    attn_out = lax.map(one_request, (queries, k_new, v_new, block_table))
    targets = ((jnp.arange(n_rows) // REQ_PER_DEV)[:, None] * BLOCKS_PER_DEV + write_ids).reshape(-1)
    new_shape = (n_rows * CHUNK_LEN // BLOCK_LEN, BLOCK_LEN, KV_HEADS, HEAD_DIM)
    k_pool_out = k_pool.at[targets].set(k_new.reshape(new_shape))
    v_pool_out = v_pool.at[targets].set(v_new.reshape(new_shape))
    return attn_out, k_pool_out, v_pool_out
```

```python
import functools

import jax
import jax.numpy as jnp
from jax import lax
from jax.experimental import pallas as pl
from jax.experimental.pallas import tpu as pltpu
from jax.sharding import PartitionSpec as P

MESH = pl.DeviceIdType.MESH
PLANES = 4
PLANE = 32
Z_CAP = 10
PAIR_CAP = 2
N_CH = 4
LOG2E = 1.4426950408889634
OFFSETS = ((0, 1), (1, 0), (0, 3), (3, 0), (1, 1), (3, 3), (1, 3), (3, 1), (0, 2), (2, 0), (1, 2), (2, 1), (3, 2), (2, 3), (2, 2), (0, 0))
ORDER = tuple((dy, dx, dc) for dc in range(2) for dy, dx in OFFSETS if (dy, dx, dc) != (0, 0, 0))


def plane_peer(pos, dy, dx, dc):
    y, x, c = lax.rem(pos // 8, 4), lax.rem(pos // 2, 4), lax.rem(pos, 2)
    return (lax.rem(y + dy, 4) * 4 + lax.rem(x + dx, 4)) * 2 + lax.rem(c + dc, 2)


def exchange_kernel(zidx_ref, bidx_ref, pool_ref, recv_ref, *scratch):
    zsend, zrecv, bsend = scratch[:N_CH], scratch[N_CH:2 * N_CH], scratch[2 * N_CH:3 * N_CH]
    zs_sem, zr_sem, bs_sem, br_sem = scratch[3 * N_CH:]
    me = lax.axis_index('pool')
    my_z, my_pos = me // PLANE, lax.rem(me, PLANE)
    base = my_z * PLANE

    barrier = pltpu.get_barrier_semaphore()
    for dz in range(1, PLANES):
        pl.semaphore_signal(barrier, inc=1, device_id=(lax.rem(my_z + dz, PLANES) * PLANE + my_pos,), device_id_type=MESH)

    @pl.loop(1, PLANE)
    def _(i):
        pl.semaphore_signal(barrier, inc=1, device_id=(base + lax.rem(my_pos + i, PLANE),), device_id_type=MESH)

    for ch in range(N_CH):
        @pl.loop(0, Z_CAP)
        def _(s):
            block = pool_ref[zidx_ref[s], ch]
            zsend[ch][s] = block
            zrecv[ch][my_z * Z_CAP + s] = block

    pl.semaphore_wait(barrier, PLANES - 1 + PLANE - 1)

    def z_copy(ch, dz):
        there = lax.rem(my_z + dz, PLANES)
        return pltpu.make_async_remote_copy(
            src_ref=zsend[ch], dst_ref=zrecv[ch].at[pl.ds(my_z * Z_CAP, Z_CAP)], send_sem=zs_sem.at[ch, dz], recv_sem=zr_sem.at[ch, dz],
            device_id=(there * PLANE + my_pos,), device_id_type=MESH)

    def b_copy(ch, peer):
        return pltpu.make_async_remote_copy(
            src_ref=bsend[ch].at[peer], dst_ref=recv_ref.at[ch, my_pos], send_sem=bs_sem.at[ch, peer], recv_sem=br_sem.at[ch, my_pos],
            device_id=(base + peer,), device_id_type=MESH)

    def b_arrival(ch, peer):
        return pltpu.make_async_remote_copy(
            src_ref=bsend[ch].at[peer], dst_ref=recv_ref.at[ch, peer], send_sem=bs_sem.at[ch, peer], recv_sem=br_sem.at[ch, peer],
            device_id=(base + peer,), device_id_type=MESH)

    for ch in range(N_CH):
        for dz in (1, 3, 2):
            z_copy(ch, dz).start()
    for ch in range(N_CH):
        for dz in (1, 3, 2):
            z_copy(ch, dz).wait_recv()

        @pl.loop(0, PLANE)
        def _(p):
            for s in range(PAIR_CAP):
                bsend[ch][p, :, s * 16:(s + 1) * 16, :] = zrecv[ch][bidx_ref[p * PAIR_CAP + s]]

        recv_ref[ch, my_pos] = bsend[ch][my_pos]
        for dy, dx, dc in ORDER:
            b_copy(ch, plane_peer(my_pos, dy, dx, dc)).start()
    for ch in range(N_CH):
        @pl.loop(1, PLANE)
        def _(i):
            b_arrival(ch, lax.rem(my_pos + i, PLANE)).wait_recv()
    for ch in range(N_CH):
        for dz in (1, 3, 2):
            z_copy(ch, dz).wait_send()

        @pl.loop(1, PLANE)
        def _(i):
            b_arrival(ch, lax.rem(my_pos + i, PLANE)).wait_send()


def exchange(zidx, bidx, pool_t):
    block = pool_t.shape[2:]
    dtype = pool_t.dtype
    pair = (block[0], PAIR_CAP * block[1], block[2])
    return pl.pallas_call(
        exchange_kernel,
        out_shape=jax.ShapeDtypeStruct((N_CH, PLANE) + pair, dtype),
        in_specs=[pl.BlockSpec(memory_space=pltpu.SMEM), pl.BlockSpec(memory_space=pltpu.SMEM), pl.BlockSpec(memory_space=pltpu.VMEM)],
        out_specs=pl.BlockSpec(memory_space=pltpu.VMEM),
        scratch_shapes=[pltpu.VMEM((Z_CAP,) + block, dtype)] * N_CH + [pltpu.VMEM((PLANES * Z_CAP,) + block, dtype)] * N_CH
        + [pltpu.VMEM((PLANE,) + pair, dtype)] * N_CH
        + [pltpu.SemaphoreType.DMA((N_CH, PLANES)), pltpu.SemaphoreType.DMA((N_CH, PLANES)),
           pltpu.SemaphoreType.DMA((N_CH, PLANE)), pltpu.SemaphoreType.DMA((N_CH, PLANE))],
        compiler_params=pltpu.CompilerParams(collective_id=0, has_side_effects=True, vmem_limit_bytes=48 << 20),
        name='exchange',
    )(zidx, bidx, pool_t)


def attention_kernel(q_ref, kv_ref, new_ref, out_ref):
    chunk_len, head_dim = q_ref.shape[0], q_ref.shape[2]
    scale = head_dim ** -0.5 * LOG2E
    group = 8
    tile = 32

    def nt(a, b):
        return lax.dot_general(a, b, (((1,), (1,)), ((), ())), preferred_element_type=jnp.float32)

    for hh in range(2):
        k_pref = kv_ref[0, :, hh].reshape(-1, head_dim)
        v_pref = kv_ref[0, :, 2 + hh].reshape(-1, head_dim)
        k_new, v_new = new_ref[0, hh], new_ref[0, 2 + hh]

        @pl.loop(0, chunk_len // tile)
        def _(t):
            q = q_ref[pl.ds(t * tile, tile), hh * group:(hh + 1) * group, :]
            q = q.astype(jnp.float32).reshape(tile * group, head_dim).astype(jnp.bfloat16)
            s_pref = nt(q, k_pref)
            s_self = nt(q, k_new)
            token = t * tile + lax.broadcasted_iota(jnp.int32, s_self.shape, 0) // group
            s_self = jnp.where(token >= lax.broadcasted_iota(jnp.int32, s_self.shape, 1), s_self, -jnp.inf)
            top = jnp.maximum(jnp.max(s_pref, axis=1, keepdims=True), jnp.max(s_self, axis=1, keepdims=True))
            e_pref = jnp.exp2((s_pref - top) * scale)
            e_self = jnp.exp2((s_self - top) * scale)
            inv = 1.0 / (jnp.sum(e_pref, axis=1, keepdims=True) + jnp.sum(e_self, axis=1, keepdims=True))
            p_pref = (e_pref * inv).astype(jnp.bfloat16)
            p_self = (e_self * inv).astype(jnp.bfloat16)
            acc = jnp.dot(p_pref, v_pref, preferred_element_type=jnp.float32) + jnp.dot(p_self, v_new, preferred_element_type=jnp.float32)
            out_ref[pl.ds(t * tile, tile), hh * group:(hh + 1) * group, :] = acc.reshape(tile, group, head_dim).astype(jnp.bfloat16)


def attention(q, kv, new):
    chunk_len, q_heads, head_dim = q.shape
    wide = q_heads // N_CH
    return pl.pallas_call(
        attention_kernel,
        grid=(N_CH,),
        out_shape=jax.ShapeDtypeStruct(q.shape, q.dtype),
        in_specs=[pl.BlockSpec((chunk_len, wide, head_dim), lambda c: (0, c, 0)),
                  pl.BlockSpec((1,) + kv.shape[1:], lambda c: (c, 0, 0, 0, 0)),
                  pl.BlockSpec((1,) + new.shape[1:], lambda c: (c, 0, 0, 0))],
        out_specs=pl.BlockSpec((chunk_len, wide, head_dim), lambda c: (0, c, 0)),
        compiler_params=pltpu.CompilerParams(vmem_limit_bytes=48 << 20),
        name='attention',
    )(q, kv, new)


def by_chunk(k, v):
    n, t, h, d = k.shape
    both = jnp.stack([k, v], axis=1).reshape(n, 2, t, N_CH, h // N_CH, d)
    return both.transpose(0, 3, 1, 4, 2, 5).reshape(n, N_CH, 2 * h // N_CH, t, d)


def plan(block_table, me, per_dev):
    n_dev = block_table.shape[0]
    owner, local = block_table // per_dev, block_table % per_dev
    col, plane = owner % PLANE, owner // PLANE
    in_col = jnp.sum((col[:, :, None] == jnp.arange(PLANE)).astype(jnp.int32), axis=1)
    own_hot = (owner.reshape(-1)[:, None] == jnp.arange(n_dev)).astype(jnp.bfloat16)
    loc_hot = (local.reshape(-1)[:, None] == jnp.arange(per_dev)).astype(jnp.bfloat16)
    named = lax.dot_general(own_hot, loc_hot, (((0,), (0,)), ((), ())), preferred_element_type=jnp.float32) > 0
    fits = (jnp.max(in_col) <= PAIR_CAP) & (jnp.max(jnp.sum(named.astype(jnp.int32), axis=1)) <= Z_CAP)
    my_z, my_pos = me // PLANE, me % PLANE
    mine = lax.dynamic_slice_in_dim(named.reshape(PLANES, PLANE, per_dev), my_pos, 1, 1)[:, 0]
    below = jnp.arange(per_dev)[:, None] < jnp.arange(per_dev)[None, :]
    rank = jnp.sum((mine[:, :, None] & below[None]).astype(jnp.int32), axis=1)
    sent = lax.dynamic_slice_in_dim(mine, my_z, 1, 0)[0]
    sent_rank = lax.dynamic_slice_in_dim(rank, my_z, 1, 0)[0]
    hit = sent[None, :] & (sent_rank[None, :] == jnp.arange(Z_CAP)[:, None])
    zidx = jnp.sum(jnp.where(hit, jnp.arange(per_dev)[None, :], 0), axis=1)
    key = plane * per_dev + local
    rows = lambda a: lax.dynamic_slice_in_dim(a, my_z * PLANE, PLANE, 0)
    match, row_key = rows(col) == my_pos, rows(key)
    n_keys = PLANES * per_dev
    first = jnp.min(jnp.where(match, row_key, n_keys - 1), axis=1)
    last = jnp.max(jnp.where(match, row_key, 0), axis=1)
    pair_key = jnp.stack([first, last], axis=1).reshape(-1)
    slot = jnp.minimum(jnp.arange(PLANES)[:, None] * Z_CAP + rank, PLANES * Z_CAP - 1).reshape(-1)
    bidx = jnp.sum(jnp.where(pair_key[:, None] == jnp.arange(n_keys)[None, :], slot[None, :], 0), axis=1)
    return fits, zidx.astype(jnp.int32), bidx.astype(jnp.int32)


def solution(mesh):
    n_dev = mesh.shape['pool']

    def padded_exchange(k_pool, v_pool, block_table):
        per_dev = k_pool.shape[0]
        n_pref = block_table.shape[1]
        my_index = lax.axis_index('pool')
        pair_cap = 2
        owners = block_table // per_dev
        owned_here = (owners == my_index).astype(jnp.int32)
        send_slot = jnp.where(owned_here > 0, jnp.cumsum(owned_here, axis=1) - 1, pair_cap)
        dest_dev = jnp.broadcast_to(jnp.arange(n_dev)[:, None], send_slot.shape)
        send_ids = jnp.zeros((n_dev, pair_cap), jnp.int32).at[dest_dev, send_slot].set(block_table % per_dev, mode='drop')
        k_recv = lax.all_to_all(k_pool[send_ids], 'pool', 0, 0, tiled=True)
        v_recv = lax.all_to_all(v_pool[send_ids], 'pool', 0, 0, tiled=True)
        my_owners = lax.dynamic_slice_in_dim(owners, my_index, 1, 0).reshape(-1)
        from_owner = (my_owners[:, None] == jnp.arange(n_dev)[None, :]).astype(jnp.int32)
        slot_rank = jnp.sum(from_owner * (jnp.cumsum(from_owner, axis=0) - 1), axis=1)
        recv_idx = my_owners * pair_cap + slot_rank
        flat = (n_dev * pair_cap,) + k_pool.shape[1:]
        pairs = by_chunk(k_recv.reshape(flat)[recv_idx], v_recv.reshape(flat)[recv_idx])
        parts, t, d = pairs.shape[2:]
        pairs = pairs.reshape(n_pref // PAIR_CAP, PAIR_CAP, N_CH, parts, t, d).transpose(2, 0, 3, 1, 4, 5)
        return pairs.reshape(N_CH, n_pref // PAIR_CAP, parts, PAIR_CAP * t, d)

    def local_step(queries, k_new, v_new, k_pool, v_pool, block_table, write_ids):
        chunk_len = queries.shape[1]
        per_dev, block_len = k_pool.shape[0], k_pool.shape[1]
        me = lax.axis_index('pool')
        fits, zidx, bidx = plan(block_table, me, per_dev)
        kv = lax.cond(
            fits,
            lambda: exchange(zidx, bidx, by_chunk(k_pool, v_pool)),
            lambda: padded_exchange(k_pool, v_pool, block_table))
        new = by_chunk(k_new, v_new)[0]
        attn_out = attention(queries[0], kv, new)[None]
        new_shape = (chunk_len // block_len, block_len) + k_new.shape[2:]
        targets = write_ids.reshape(-1)
        k_pool_out = k_pool.at[targets].set(k_new.reshape(new_shape))
        v_pool_out = v_pool.at[targets].set(v_new.reshape(new_shape))
        return attn_out, k_pool_out, v_pool_out

    row_spec = P('pool')
    return jax.shard_map(local_step, mesh=mesh, in_specs=(row_spec, row_spec, row_spec, row_spec, row_spec, P(), row_spec), out_specs=(row_spec, row_spec, row_spec), check_vma=False)
```

```python
import jax
import jax.numpy as jnp
from jax import lax
from jax.experimental import pallas as pl
from jax.experimental.pallas import tpu as pltpu
from jax.sharding import PartitionSpec as P

MESH = pl.DeviceIdType.MESH
PLANES = 4
PLANE = 32
Z_CAP = 10
PAIR_CAP = 2
N_CH = 8
GROUP = 8
TILE = 32
LOG2E = 1.4426950408889634
OFFSETS = ((0, 1), (1, 0), (0, 3), (3, 0), (1, 1), (3, 3), (1, 3), (3, 1), (0, 2), (2, 0), (1, 2), (2, 1), (3, 2), (2, 3), (2, 2), (0, 0))
ORDER = tuple((dy, dx, dc) for dc in range(2) for dy, dx in OFFSETS if (dy, dx, dc) != (0, 0, 0))


def plane_peer(pos, dy, dx, dc):
    y, x, c = lax.rem(pos // 8, 4), lax.rem(pos // 2, 4), lax.rem(pos, 2)
    return (lax.rem(y + dy, 4) * 4 + lax.rem(x + dx, 4)) * 2 + lax.rem(c + dc, 2)


def attend_head(q_ref, kv, new, out_ref, ch):
    chunk_len, head_dim = q_ref.shape[0], q_ref.shape[2]
    scale = head_dim ** -0.5 * LOG2E
    heads = pl.ds(pl.multiple_of(ch * GROUP, GROUP), GROUP)
    k_pref, v_pref = kv(0), kv(1)
    k_new, v_new = new(0), new(1)

    def nt(a, b):
        return lax.dot_general(a, b, (((1,), (1,)), ((), ())), preferred_element_type=jnp.float32)

    @pl.loop(0, chunk_len // TILE)
    def _(t):
        tokens = pl.ds(t * TILE, TILE)
        q = q_ref[tokens, heads, :].astype(jnp.float32).reshape(TILE * GROUP, head_dim).astype(jnp.bfloat16)
        s_pref = nt(q, k_pref)
        s_self = nt(q, k_new)
        token = t * TILE + lax.broadcasted_iota(jnp.int32, s_self.shape, 0) // GROUP
        s_self = jnp.where(token >= lax.broadcasted_iota(jnp.int32, s_self.shape, 1), s_self, -jnp.inf)
        top = jnp.maximum(jnp.max(s_pref, axis=1, keepdims=True), jnp.max(s_self, axis=1, keepdims=True))
        e_pref = jnp.exp2((s_pref - top) * scale)
        e_self = jnp.exp2((s_self - top) * scale)
        inv = 1.0 / (jnp.sum(e_pref, axis=1, keepdims=True) + jnp.sum(e_self, axis=1, keepdims=True))
        p_pref = (e_pref * inv).astype(jnp.bfloat16)
        p_self = (e_self * inv).astype(jnp.bfloat16)
        acc = jnp.dot(p_pref, v_pref, preferred_element_type=jnp.float32) + jnp.dot(p_self, v_new, preferred_element_type=jnp.float32)
        out_ref[tokens, heads, :] = acc.reshape(TILE, GROUP, head_dim).astype(jnp.bfloat16)


def exchange_kernel(zidx_ref, bidx_ref, q_ref, pool_ref, new_ref, out_ref, recv_ref, *scratch):
    zsend, zrecv, bsend = scratch[:N_CH], scratch[N_CH:2 * N_CH], scratch[2 * N_CH:3 * N_CH]
    zs_sem, zr_sem, bs_sem, br_sem = scratch[3 * N_CH:]
    me = lax.axis_index('pool')
    my_z, my_pos = me // PLANE, lax.rem(me, PLANE)
    base = my_z * PLANE
    head_dim = q_ref.shape[2]

    barrier = pltpu.get_barrier_semaphore()
    for dz in range(1, PLANES):
        pl.semaphore_signal(barrier, inc=1, device_id=(lax.rem(my_z + dz, PLANES) * PLANE + my_pos,), device_id_type=MESH)

    @pl.loop(1, PLANE)
    def _(i):
        pl.semaphore_signal(barrier, inc=1, device_id=(base + lax.rem(my_pos + i, PLANE),), device_id_type=MESH)

    for ch in range(N_CH):
        @pl.loop(0, Z_CAP)
        def _(s):
            block = pool_ref[zidx_ref[s], ch]
            zsend[ch][s] = block
            zrecv[ch][my_z * Z_CAP + s] = block

    pl.semaphore_wait(barrier, PLANES - 1 + PLANE - 1)

    def z_copy(ch, dz):
        there = lax.rem(my_z + dz, PLANES)
        return pltpu.make_async_remote_copy(
            src_ref=zsend[ch], dst_ref=zrecv[ch].at[pl.ds(my_z * Z_CAP, Z_CAP)], send_sem=zs_sem.at[ch, dz], recv_sem=zr_sem.at[ch, dz],
            device_id=(there * PLANE + my_pos,), device_id_type=MESH)

    def b_copy(ch, peer):
        return pltpu.make_async_remote_copy(
            src_ref=bsend[ch].at[peer], dst_ref=recv_ref.at[ch, my_pos], send_sem=bs_sem.at[ch, peer], recv_sem=br_sem.at[ch, my_pos],
            device_id=(base + peer,), device_id_type=MESH)

    def b_arrival(ch, peer):
        return pltpu.make_async_remote_copy(
            src_ref=bsend[0].at[peer], dst_ref=recv_ref.at[ch, peer], send_sem=bs_sem.at[ch, peer], recv_sem=br_sem.at[ch, peer],
            device_id=(base + peer,), device_id_type=MESH)

    for ch in range(N_CH):
        for dz in (1, 3, 2):
            z_copy(ch, dz).start()
    for ch in range(N_CH):
        for dz in (1, 3, 2):
            z_copy(ch, dz).wait_recv()

        @pl.loop(0, PLANE)
        def _(p):
            for s in range(PAIR_CAP):
                bsend[ch][p, :, s * 16:(s + 1) * 16, :] = zrecv[ch][bidx_ref[p * PAIR_CAP + s]]

        recv_ref[ch, my_pos] = bsend[ch][my_pos]
        for dy, dx, dc in ORDER:
            b_copy(ch, plane_peer(my_pos, dy, dx, dc)).start()

    @pl.loop(0, N_CH)
    def _(ch):
        @pl.loop(1, PLANE)
        def _(i):
            b_arrival(ch, lax.rem(my_pos + i, PLANE)).wait_recv()

        attend_head(q_ref, lambda part: recv_ref[ch, :, part].reshape(-1, head_dim), lambda part: new_ref[ch, part], out_ref, ch)

    for ch in range(N_CH):
        for dz in (1, 3, 2):
            z_copy(ch, dz).wait_send()

        @pl.loop(1, PLANE)
        def _(i):
            b_arrival(ch, lax.rem(my_pos + i, PLANE)).wait_send()


def exchange_attention(zidx, bidx, q, pool_t, new):
    block = pool_t.shape[2:]
    dtype = pool_t.dtype
    pair = (block[0], PAIR_CAP * block[1], block[2])
    vmem, smem = pl.BlockSpec(memory_space=pltpu.VMEM), pl.BlockSpec(memory_space=pltpu.SMEM)
    return pl.pallas_call(
        exchange_kernel,
        out_shape=jax.ShapeDtypeStruct(q.shape, dtype),
        in_specs=[smem, smem, vmem, vmem, vmem],
        out_specs=vmem,
        scratch_shapes=[pltpu.VMEM((N_CH, PLANE) + pair, dtype)]
        + [pltpu.VMEM((Z_CAP,) + block, dtype)] * N_CH + [pltpu.VMEM((PLANES * Z_CAP,) + block, dtype)] * N_CH
        + [pltpu.VMEM((PLANE,) + pair, dtype)] * N_CH
        + [pltpu.SemaphoreType.DMA((N_CH, PLANES)), pltpu.SemaphoreType.DMA((N_CH, PLANES)),
           pltpu.SemaphoreType.DMA((N_CH, PLANE)), pltpu.SemaphoreType.DMA((N_CH, PLANE))],
        compiler_params=pltpu.CompilerParams(collective_id=0, has_side_effects=True, vmem_limit_bytes=56 << 20),
        name='exchange_attention',
    )(zidx, bidx, q, pool_t, new)


def attention_kernel(q_ref, kv_ref, new_ref, out_ref):
    head_dim = q_ref.shape[2]
    attend_head(q_ref, lambda part: kv_ref[0, :, part].reshape(-1, head_dim), lambda part: new_ref[0, part], out_ref, 0)


def attention(q, kv, new):
    chunk_len, q_heads, head_dim = q.shape
    return pl.pallas_call(
        attention_kernel,
        grid=(N_CH,),
        out_shape=jax.ShapeDtypeStruct(q.shape, q.dtype),
        in_specs=[pl.BlockSpec((chunk_len, GROUP, head_dim), lambda c: (0, c, 0)),
                  pl.BlockSpec((1,) + kv.shape[1:], lambda c: (c, 0, 0, 0, 0)),
                  pl.BlockSpec((1,) + new.shape[1:], lambda c: (c, 0, 0, 0))],
        out_specs=pl.BlockSpec((chunk_len, GROUP, head_dim), lambda c: (0, c, 0)),
        compiler_params=pltpu.CompilerParams(vmem_limit_bytes=48 << 20),
        name='attention',
    )(q, kv, new)


def by_chunk(k, v):
    n, t, h, d = k.shape
    both = jnp.stack([k, v], axis=1).reshape(n, 2, t, N_CH, h // N_CH, d)
    return both.transpose(0, 3, 1, 4, 2, 5).reshape(n, N_CH, 2 * h // N_CH, t, d)


def plan(block_table, me, per_dev):
    n_dev = block_table.shape[0]
    owner, local = block_table // per_dev, block_table % per_dev
    col, plane = owner % PLANE, owner // PLANE
    in_col = jnp.sum((col[:, :, None] == jnp.arange(PLANE)).astype(jnp.int32), axis=1)
    own_hot = (owner.reshape(-1)[:, None] == jnp.arange(n_dev)).astype(jnp.bfloat16)
    loc_hot = (local.reshape(-1)[:, None] == jnp.arange(per_dev)).astype(jnp.bfloat16)
    named = lax.dot_general(own_hot, loc_hot, (((0,), (0,)), ((), ())), preferred_element_type=jnp.float32) > 0
    fits = (jnp.max(in_col) <= PAIR_CAP) & (jnp.max(jnp.sum(named.astype(jnp.int32), axis=1)) <= Z_CAP)
    my_z, my_pos = me // PLANE, me % PLANE
    mine = lax.dynamic_slice_in_dim(named.reshape(PLANES, PLANE, per_dev), my_pos, 1, 1)[:, 0]
    below = jnp.arange(per_dev)[:, None] < jnp.arange(per_dev)[None, :]
    rank = jnp.sum((mine[:, :, None] & below[None]).astype(jnp.int32), axis=1)
    sent = lax.dynamic_slice_in_dim(mine, my_z, 1, 0)[0]
    sent_rank = lax.dynamic_slice_in_dim(rank, my_z, 1, 0)[0]
    hit = sent[None, :] & (sent_rank[None, :] == jnp.arange(Z_CAP)[:, None])
    zidx = jnp.sum(jnp.where(hit, jnp.arange(per_dev)[None, :], 0), axis=1)
    key = plane * per_dev + local
    rows = lambda a: lax.dynamic_slice_in_dim(a, my_z * PLANE, PLANE, 0)
    match, row_key = rows(col) == my_pos, rows(key)
    n_keys = PLANES * per_dev
    first = jnp.min(jnp.where(match, row_key, n_keys - 1), axis=1)
    last = jnp.max(jnp.where(match, row_key, 0), axis=1)
    pair_key = jnp.stack([first, last], axis=1).reshape(-1)
    slot = jnp.minimum(jnp.arange(PLANES)[:, None] * Z_CAP + rank, PLANES * Z_CAP - 1).reshape(-1)
    bidx = jnp.sum(jnp.where(pair_key[:, None] == jnp.arange(n_keys)[None, :], slot[None, :], 0), axis=1)
    return fits, zidx.astype(jnp.int32), bidx.astype(jnp.int32)


def solution(mesh):
    n_dev = mesh.shape['pool']

    def padded_exchange(k_pool, v_pool, block_table):
        per_dev = k_pool.shape[0]
        n_pref = block_table.shape[1]
        my_index = lax.axis_index('pool')
        pair_cap = 2
        owners = block_table // per_dev
        owned_here = (owners == my_index).astype(jnp.int32)
        send_slot = jnp.where(owned_here > 0, jnp.cumsum(owned_here, axis=1) - 1, pair_cap)
        dest_dev = jnp.broadcast_to(jnp.arange(n_dev)[:, None], send_slot.shape)
        send_ids = jnp.zeros((n_dev, pair_cap), jnp.int32).at[dest_dev, send_slot].set(block_table % per_dev, mode='drop')
        k_recv = lax.all_to_all(k_pool[send_ids], 'pool', 0, 0, tiled=True)
        v_recv = lax.all_to_all(v_pool[send_ids], 'pool', 0, 0, tiled=True)
        my_owners = lax.dynamic_slice_in_dim(owners, my_index, 1, 0).reshape(-1)
        from_owner = (my_owners[:, None] == jnp.arange(n_dev)[None, :]).astype(jnp.int32)
        slot_rank = jnp.sum(from_owner * (jnp.cumsum(from_owner, axis=0) - 1), axis=1)
        recv_idx = my_owners * pair_cap + slot_rank
        flat = (n_dev * pair_cap,) + k_pool.shape[1:]
        pairs = by_chunk(k_recv.reshape(flat)[recv_idx], v_recv.reshape(flat)[recv_idx])
        parts, t, d = pairs.shape[2:]
        pairs = pairs.reshape(n_pref // PAIR_CAP, PAIR_CAP, N_CH, parts, t, d).transpose(2, 0, 3, 1, 4, 5)
        return pairs.reshape(N_CH, n_pref // PAIR_CAP, parts, PAIR_CAP * t, d)

    def local_step(queries, k_new, v_new, k_pool, v_pool, block_table, write_ids):
        chunk_len = queries.shape[1]
        per_dev, block_len = k_pool.shape[0], k_pool.shape[1]
        me = lax.axis_index('pool')
        fits, zidx, bidx = plan(block_table, me, per_dev)
        new = by_chunk(k_new, v_new)[0]
        attn_out = lax.cond(
            fits,
            lambda: exchange_attention(zidx, bidx, queries[0], by_chunk(k_pool, v_pool), new),
            lambda: attention(queries[0], padded_exchange(k_pool, v_pool, block_table), new))[None]
        new_shape = (chunk_len // block_len, block_len) + k_new.shape[2:]
        targets = write_ids.reshape(-1)
        k_pool_out = k_pool.at[targets].set(k_new.reshape(new_shape))
        v_pool_out = v_pool.at[targets].set(v_new.reshape(new_shape))
        return attn_out, k_pool_out, v_pool_out

    row_spec = P('pool')
    return jax.shard_map(local_step, mesh=mesh, in_specs=(row_spec, row_spec, row_spec, row_spec, row_spec, P(), row_spec), out_specs=(row_spec, row_spec, row_spec), check_vma=False)
```

```python
import jax
import jax.numpy as jnp
from jax import lax
from jax.experimental import pallas as pl
from jax.experimental.pallas import tpu as pltpu
from jax.sharding import PartitionSpec as P

MESH = pl.DeviceIdType.MESH
PLANES = 4
PLANE = 32
Z_CAP = 10
PAIR_CAP = 2
N_CH = 8
GROUP = 8
TILE = 64
LOG2E = 1.4426950408889634
RING = 4
GROUP_CAP = 10
LAG = 3
STEPS = (1, 3, 2)


def attend_head(q_ref, kv, new, out_ref, ch):
    chunk_len, head_dim = q_ref.shape[0], q_ref.shape[2]
    scale = head_dim ** -0.5 * LOG2E
    heads = pl.ds(ch * GROUP, GROUP)
    k_pref, v_pref = kv(0), kv(1)
    k_new, v_new = new(0), new(1)

    def nt(a, b):
        return lax.dot_general(a, b, (((1,), (1,)), ((), ())), preferred_element_type=jnp.float32)

    @pl.loop(0, chunk_len // TILE)
    def _(t):
        tokens = pl.ds(t * TILE, TILE)
        q = q_ref[tokens, heads, :].astype(jnp.float32).reshape(TILE * GROUP, head_dim).astype(jnp.bfloat16)
        s_pref = nt(q, k_pref)
        s_self = nt(q, k_new)
        token = t * TILE + lax.broadcasted_iota(jnp.int32, s_self.shape, 0) // GROUP
        s_self = jnp.where(token >= lax.broadcasted_iota(jnp.int32, s_self.shape, 1), s_self, -jnp.inf)
        top = jnp.maximum(jnp.max(s_pref, axis=1, keepdims=True), jnp.max(s_self, axis=1, keepdims=True))
        e_pref = jnp.exp2((s_pref - top) * scale)
        e_self = jnp.exp2((s_self - top) * scale)
        inv = 1.0 / (jnp.sum(e_pref, axis=1, keepdims=True) + jnp.sum(e_self, axis=1, keepdims=True))
        p_pref = (e_pref * inv).astype(jnp.bfloat16)
        p_self = (e_self * inv).astype(jnp.bfloat16)
        acc = jnp.dot(p_pref, v_pref, preferred_element_type=jnp.float32) + jnp.dot(p_self, v_new, preferred_element_type=jnp.float32)
        out_ref[tokens, heads, :] = acc.reshape(TILE, GROUP, head_dim).astype(jnp.bfloat16)


def head_major(src, wide, store, blocks):
    for i in range(blocks):
        tokens, heads, dim = wide.shape[1:]
        slot = i % wide.shape[0]
        wide[slot] = src(i).astype(jnp.float32)
        flat = wide.at[slot].reshape(tokens * heads, dim)
        for h in range(heads):
            store(i, h, flat[pl.ds(h, tokens, stride=heads), :].astype(jnp.bfloat16))


def prepare_kernel(wid_ref, table_ref, k_pool_hbm, v_pool_hbm, k_new_hbm, v_new_hbm, k_out_hbm, v_out_hbm, fits_ref, first_ref, second_ref, zsend_ref,
                   k_pool, v_pool, k_new, v_new, named, idx_vec, idx_smem, wide, in_sem, out_sem, idx_sem):
    me = lax.axis_index('pool')
    my_z, my_pos = me // PLANE, lax.rem(me, PLANE)
    per_dev = k_pool.shape[0]
    n_pref, n_row = table_ref.shape
    n_dev = n_row
    loads = [pltpu.make_async_copy(src, dst, in_sem.at[i]) for i, (src, dst) in enumerate(
        ((k_pool_hbm, k_pool), (v_pool_hbm, v_pool), (k_new_hbm, k_new), (v_new_hbm, v_new)))]
    for copy in loads:
        copy.start()

    def iota(shape, dim):
        return lax.broadcasted_iota(jnp.int32, shape, dim)

    def nt(x, y):
        return lax.dot_general(x, y, (((1,), (1,)), ((), ())), preferred_element_type=jnp.float32)

    def one_hot(row, rows):
        return jnp.where(iota((rows, n_row), 0) == row, 1.0, 0.0).astype(jnp.bfloat16)

    counts = jnp.zeros((n_dev, per_dev), jnp.float32)
    step = 8
    for e in range(0, n_pref, step):
        rows = [table_ref[e + i:e + i + 1, :] for i in range(step)]
        hot_owner = jnp.concatenate([one_hot(row // per_dev, n_dev) for row in rows], axis=1)
        hot_local = jnp.concatenate([one_hot(row % per_dev, per_dev) for row in rows], axis=1)
        counts = counts + nt(hot_owner, hot_local)
    is_named = jnp.where(counts > 0, 1.0, 0.0)
    named[...] = is_named
    most_named = jnp.max(jnp.sum(is_named, axis=1, keepdims=True), axis=0, keepdims=True)

    table = table_ref[...]
    owner, local = table // per_dev, table % per_dev
    col, plane = owner % PLANE, owner // PLANE
    most_in_col = jnp.zeros((1, n_row), jnp.int32)
    for c in range(PLANE):
        most_in_col = jnp.maximum(most_in_col, jnp.sum(jnp.where(col == c, 1, 0), axis=0, keepdims=True))
    most_in_col = jnp.max(most_in_col, axis=1, keepdims=True)

    key = plane * per_dev + local
    n_key = PLANES * per_dev

    def ends(q):
        match = col == q
        return (jnp.min(jnp.where(match, key, n_key - 1), axis=0, keepdims=True), jnp.max(jnp.where(match, key, 0), axis=0, keepdims=True))

    def flag(mask):
        return jnp.where(mask, 1.0, 0.0).astype(jnp.bfloat16)

    def members(n_group, plane_of, index_of):
        group, row = iota((n_group, n_row), 0), iota((n_group, n_row), 1)
        at = jnp.where(group // RING % 2 == 0, row // 8 % RING, row // 2 % RING)
        return flag((row // PLANE == plane_of(group)) & (at == index_of(group)))

    all_groups = members(2 * RING * PLANES, lambda g: g // (2 * RING), lambda g: g % RING)

    def widest(q, most):
        first, last = ends(q)
        named_by = nt(all_groups, flag((iota((n_key, n_row), 0) == first) | (iota((n_key, n_row), 0) == last)))
        return jnp.maximum(most, jnp.sum(jnp.where(named_by > 0, 1.0, 0.0), axis=1, keepdims=True))

    most_in_group = lax.fori_loop(0, PLANE, widest, jnp.zeros((2 * RING * PLANES, 1), jnp.float32), unroll=4)
    most_in_group = jnp.max(most_in_group, axis=0, keepdims=True)
    fits = jnp.where((most_named <= Z_CAP) & (most_in_col <= PAIR_CAP) & (most_in_group <= GROUP_CAP), 1, 0)
    fits_ref[...] = jnp.broadcast_to(fits, fits_ref.shape)

    mine = jnp.concatenate([named[pl.ds(z * PLANE + my_pos, 1), :] for z in range(PLANES)], axis=0)
    before = jnp.where(iota((per_dev, per_dev), 0) < iota((per_dev, per_dev), 1), 1.0, 0.0).astype(jnp.bfloat16)
    rank = jnp.dot(mine.astype(jnp.bfloat16), before, preferred_element_type=jnp.float32)
    own = iota(rank.shape, 0) == my_z
    own_rank = jnp.sum(jnp.where(own & (mine > 0), rank, 0.0) + jnp.where(own & (mine == 0), 1000.0, 0.0), axis=0, keepdims=True)
    hit = iota((16, per_dev), 0).astype(jnp.float32) == own_rank
    chosen = jnp.sum(jnp.where(hit, iota((16, per_dev), 1), 0), axis=1, keepdims=True)
    idx_vec[...] = jnp.broadcast_to(chosen, idx_vec.shape)
    to_smem = pltpu.make_async_copy(idx_vec, idx_smem, idx_sem)
    to_smem.start()

    slot = jnp.minimum(rank, Z_CAP - 1.0) + (iota(rank.shape, 0) * Z_CAP).astype(jnp.float32)
    slot_row = jnp.zeros((1, n_key), jnp.float32)
    for z in range(PLANES):
        place = flag(iota((per_dev, n_key), 1) == iota((per_dev, n_key), 0) + z * per_dev)
        slot_row = slot_row + jnp.dot(slot[z:z + 1].astype(jnp.bfloat16), place, preferred_element_type=jnp.float32)
    groups = members(2 * RING, lambda g: my_z, lambda g: g % RING)
    before_key = flag(iota((n_key, n_key), 0) < iota((n_key, n_key), 1))
    my_y, my_x, my_c = my_pos // 8, lax.rem(my_pos // 2, RING), lax.rem(my_pos, 2)

    def lists(q):
        hots = [flag(iota((n_key, n_row), 0) == end) for end in ends(q)]
        listed = jnp.where(nt(groups, hots[0]) + nt(groups, hots[1]) > 0, 1.0, 0.0)
        return hots, listed, jnp.dot(listed.astype(jnp.bfloat16), before_key, preferred_element_type=jnp.float32)

    _, listed, place = lists(my_pos)
    first_step = jnp.zeros((2 * RING, 128), jnp.int32)
    for i in range(GROUP_CAP):
        at = jnp.sum(jnp.where((listed > 0) & (place == i), slot_row, 0.0), axis=1, keepdims=True).astype(jnp.int32)
        first_step = jnp.where(iota(first_step.shape, 1) == i, at, first_step)
    first_ref[...] = first_step
    for part in range(2):
        for src in range(RING):
            q = (src * 8 + my_x * 2 + my_c) if part == 0 else (my_y * 8 + src * 2 + my_c)
            mine_at = my_y if part == 0 else RING + my_x
            hots, listed, place = lists(q)
            for end in range(PAIR_CAP):
                found = jnp.dot(place.astype(jnp.bfloat16), hots[end], preferred_element_type=jnp.float32)
                found = jnp.sum(jnp.where(iota(found.shape, 0) == mine_at, found, 0.0), axis=0, keepdims=True)
                line = (part * RING + src) * PAIR_CAP + end
                second_ref[line:line + 1, :] = jnp.minimum(found.astype(jnp.int32), GROUP_CAP - 1) + src * GROUP_CAP

    for copy in loads:
        copy.wait()
    pools = [pltpu.make_async_copy(src, dst, out_sem.at[i]) for i, (src, dst) in enumerate(((k_pool, k_out_hbm), (v_pool, v_out_hbm)))]
    for copy in pools:
        copy.start()
    to_smem.wait()
    for part, pool in enumerate((k_pool, v_pool)):
        def store(i, h, x):
            zsend_ref[h, i, part] = x
        head_major(lambda i: pool[idx_smem[i, 0]], wide, store, Z_CAP)
    for copy in pools:
        copy.wait()
    writes = []
    for i in range(k_new.shape[0]):
        for part, (src, dst) in enumerate(((k_new, k_out_hbm), (v_new, v_out_hbm))):
            writes.append(pltpu.make_async_copy(src.at[i], dst.at[wid_ref[0, i]], in_sem.at[2 * i + part]))
            writes[-1].start()
    for copy in writes:
        copy.wait()


def prepare(write_ids, table_t, k_pool, v_pool, k_new, v_new):
    per_dev, tokens, heads, dim = k_pool.shape
    n_row = table_t.shape[1]
    new_blocks = k_new.shape[0]
    vmem, smem, hbm = (pl.BlockSpec(memory_space=m) for m in (pltpu.VMEM, pltpu.SMEM, pl.ANY))
    return pl.pallas_call(
        prepare_kernel,
        out_shape=[jax.ShapeDtypeStruct(k_pool.shape, k_pool.dtype), jax.ShapeDtypeStruct(v_pool.shape, v_pool.dtype),
                   jax.ShapeDtypeStruct((8, 128), jnp.int32), jax.ShapeDtypeStruct((2 * RING, 128), jnp.int32),
                   jax.ShapeDtypeStruct((2 * RING * PAIR_CAP, n_row), jnp.int32),
                   jax.ShapeDtypeStruct((N_CH, Z_CAP, 2, tokens, dim), k_pool.dtype)],
        in_specs=[smem, vmem, hbm, hbm, hbm, hbm],
        out_specs=[hbm, hbm, vmem, vmem, vmem, vmem],
        scratch_shapes=[pltpu.VMEM(k_pool.shape, k_pool.dtype), pltpu.VMEM(k_pool.shape, k_pool.dtype),
                        pltpu.VMEM(k_new.shape, k_pool.dtype), pltpu.VMEM(k_new.shape, k_pool.dtype),
                        pltpu.VMEM((n_row, per_dev), jnp.float32), pltpu.VMEM((16, 128), jnp.int32), pltpu.SMEM((16, 128), jnp.int32),
                        pltpu.VMEM((4, tokens, heads, dim), jnp.float32),
                        pltpu.SemaphoreType.DMA((2 * new_blocks,)), pltpu.SemaphoreType.DMA((2,)), pltpu.SemaphoreType.DMA],
        compiler_params=pltpu.CompilerParams(vmem_limit_bytes=32 << 20),
        name='prepare',
    )(write_ids, table_t, k_pool, v_pool, k_new, v_new)


def exchange_kernel(first_ref, second_ref, q_hbm, zsend_hbm, k_new_hbm, v_new_hbm, out_hbm, q_ref, out_ref, recv_k, recv_v, k_new, v_new,
                    new_t, wide, zsend, *scratch):
    zrecv, send1, recv1, send2 = (scratch[:N_CH], scratch[N_CH:3 * N_CH], scratch[3 * N_CH:5 * N_CH], scratch[5 * N_CH:7 * N_CH])
    zs_sem, zr_sem, s1_sem, r1_sem, s2_sem, r2_sem, in_sem, out_sem = scratch[7 * N_CH:]
    me = lax.axis_index('pool')
    my_z, my_pos = me // PLANE, lax.rem(me, PLANE)
    base = my_z * PLANE
    y, x, c = my_pos // 8, lax.rem(my_pos // 2, RING), lax.rem(my_pos, 2)
    head_dim = q_ref.shape[2]

    def z_peer(d):
        return lax.rem(my_z + d, PLANES) * PLANE + my_pos

    def y_peer(d, dc):
        return base + lax.rem(y + d, RING) * 8 + x * 2 + lax.rem(c + dc, 2)

    def x_peer(d, dc):
        return base + y * 8 + lax.rem(x + d, RING) * 2 + lax.rem(c + dc, 2)

    barrier = pltpu.get_barrier_semaphore()
    peers = [z_peer(d) for d in STEPS] + [peer(d, dc) for d in STEPS for dc in range(2) for peer in (y_peer, x_peer)] + [y_peer(0, 1)]
    for peer in peers:
        pl.semaphore_signal(barrier, inc=1, device_id=(peer,), device_id_type=MESH)

    loads = [pltpu.make_async_copy(src, dst, in_sem.at[i]) for i, (src, dst) in enumerate(
        ((zsend_hbm, zsend), (k_new_hbm, k_new), (v_new_hbm, v_new), (q_hbm, q_ref)))]
    for copy in loads:
        copy.start()

    def remote(src, dst, send_sem, recv_sem, peer):
        return pltpu.make_async_remote_copy(
            src_ref=src, dst_ref=dst, send_sem=send_sem, recv_sem=recv_sem, device_id=(peer,), device_id_type=MESH)

    def wait_bytes(ref, sem):
        pltpu.make_async_copy(ref, ref, sem).wait()

    def z_wait(ch, sem):
        wait_bytes(zrecv[ch].at[pl.ds(0, (PLANES - 1) * Z_CAP)], sem.at[ch])

    def wait1(i, sem):
        wait_bytes(recv1[i].at[pl.ds(0, (RING - 1) * GROUP_CAP)], sem.at[i])

    def wait2(i, sem):
        wait_bytes(send2[i].at[pl.ds(0, 2 * RING - 1)], sem.at[i])

    def step1(ch):
        for part in range(2):
            i = 2 * ch + part
            for g in range(RING):
                for s in range(GROUP_CAP):
                    send1[i][g, s] = zrecv[ch][first_ref[part * RING + g, s], part]
            mine = y if part == 0 else x
            recv1[i][pl.ds(mine * GROUP_CAP, GROUP_CAP)] = send1[i][mine]
        for d in STEPS:
            for part in range(2):
                i = 2 * ch + part
                mine, peer = (y, y_peer(d, 0)) if part == 0 else (x, x_peer(d, 0))
                remote(send1[i].at[lax.rem(mine + d, RING)], recv1[i].at[pl.ds(mine * GROUP_CAP, GROUP_CAP)],
                       s1_sem.at[i], r1_sem.at[i], peer).start()

    def step2(ch):
        for part in range(2):
            i = 2 * ch + part
            wait1(i, r1_sem)

            @pl.loop(0, RING)
            def _(to):
                for core in range(2):
                    row = base + ((y * 8 + to * 2) if part == 0 else (to * 8 + x * 2)) + core
                    for src in range(RING):
                        for end in range(PAIR_CAP):
                            send2[i][to * 2 + core, src, end * 16:(end + 1) * 16, :] = recv1[i][second_ref[(part * RING + src) * PAIR_CAP + end, row]]

        recv_k[ch, :, x, c] = send2[2 * ch][x * 2 + c]
        recv_v[ch, y, :, c] = send2[2 * ch + 1][y * 2 + c]
        for d in STEPS + (0,):
            for dc in range(2):
                for part in range(2):
                    if (d, dc) == (0, 0):
                        continue
                    i = 2 * ch + part
                    mine, peer = (x, x_peer(d, dc)) if part == 0 else (y, y_peer(d, dc))
                    dst = recv_k.at[ch, :, x, c] if part == 0 else recv_v.at[ch, y, :, c]
                    remote(send2[i].at[lax.rem(mine + d, RING) * 2 + lax.rem(c + dc, 2)], dst, s2_sem.at[i], r2_sem.at[i], peer).start()

    def out_copy(ch):
        heads = pl.ds(ch * GROUP, GROUP)
        return pltpu.make_async_copy(out_ref.at[:, heads, :], out_hbm.at[:, heads, :], out_sem.at[ch])

    def attend(ch):
        wait2(2 * ch, r2_sem)
        wait2(2 * ch + 1, r2_sem)
        recv = (recv_k, recv_v)
        attend_head(q_ref, lambda part: recv[part][ch].reshape(-1, head_dim), lambda part: new_t[ch, part], out_ref, ch)
        out_copy(ch).start()

    loads[0].wait()
    pl.semaphore_wait(barrier, len(peers))
    for ch in range(N_CH):
        for d in STEPS:
            remote(zsend.at[ch], zrecv[ch].at[pl.ds(my_z * Z_CAP, Z_CAP)], zs_sem.at[ch], zr_sem.at[ch], z_peer(d)).start()
    for ch in range(N_CH):
        zrecv[ch][pl.ds(my_z * Z_CAP, Z_CAP)] = zsend[ch]
    for part, block in enumerate((k_new, v_new)):
        loads[1 + part].wait()

        def store(i, h, x):
            new_t[h, part, i * 16:(i + 1) * 16, :] = x
        head_major(lambda i: block[i], wide, store, block.shape[0])
    loads[3].wait()
    for t in range(N_CH + LAG):
        if t < N_CH:
            z_wait(t, zr_sem)
            step1(t)
        if 1 <= t <= N_CH:
            step2(t - 1)
        if t >= LAG:
            attend(t - LAG)
    for ch in range(N_CH):
        z_wait(ch, zs_sem)
        out_copy(ch).wait()
    for i in range(2 * N_CH):
        wait1(i, s1_sem)
        wait2(i, s2_sem)


def exchange_attention(first, second, q, zsend, k_new, v_new):
    tokens, dim = zsend.shape[3:]
    dtype = q.dtype
    hbm, smem = pl.BlockSpec(memory_space=pl.ANY), pl.BlockSpec(memory_space=pltpu.SMEM)
    recv = pltpu.VMEM((N_CH, RING, RING, 2, PAIR_CAP * tokens, dim), dtype)
    return pl.pallas_call(
        exchange_kernel,
        out_shape=jax.ShapeDtypeStruct(q.shape, dtype),
        in_specs=[smem, smem, hbm, hbm, hbm, hbm],
        out_specs=hbm,
        scratch_shapes=[pltpu.VMEM(q.shape, dtype), pltpu.VMEM(q.shape, dtype), recv, recv,
                        pltpu.VMEM(k_new.shape, dtype), pltpu.VMEM(v_new.shape, dtype), pltpu.VMEM((N_CH, 2, q.shape[0], q.shape[2]), dtype),
                        pltpu.VMEM((4,) + k_new.shape[1:], jnp.float32), pltpu.VMEM(zsend.shape, dtype)]
        + [pltpu.VMEM((PLANES * Z_CAP, 2, tokens, dim), dtype)] * N_CH
        + [pltpu.VMEM((RING, GROUP_CAP, tokens, dim), dtype)] * (2 * N_CH)
        + [pltpu.VMEM((RING * GROUP_CAP, tokens, dim), dtype)] * (2 * N_CH)
        + [pltpu.VMEM((2 * RING, RING, PAIR_CAP * tokens, dim), dtype)] * (2 * N_CH)
        + [pltpu.SemaphoreType.DMA((N_CH,))] * 2 + [pltpu.SemaphoreType.DMA((2 * N_CH,))] * 4 + [pltpu.SemaphoreType.DMA((N_CH,))] * 2,
        compiler_params=pltpu.CompilerParams(collective_id=0, has_side_effects=True, vmem_limit_bytes=56 << 20),
        name='exchange_attention',
    )(first, second, q, zsend, k_new, v_new)


def attention_kernel(q_ref, kv_ref, new_ref, out_ref):
    head_dim = q_ref.shape[2]
    attend_head(q_ref, lambda part: kv_ref[0, :, part].reshape(-1, head_dim), lambda part: new_ref[0, part], out_ref, 0)


def attention(q, kv, new):
    chunk_len, q_heads, head_dim = q.shape
    return pl.pallas_call(
        attention_kernel,
        grid=(N_CH,),
        out_shape=jax.ShapeDtypeStruct(q.shape, q.dtype),
        in_specs=[pl.BlockSpec((chunk_len, GROUP, head_dim), lambda c: (0, c, 0)),
                  pl.BlockSpec((1,) + kv.shape[1:], lambda c: (c, 0, 0, 0, 0)),
                  pl.BlockSpec((1,) + new.shape[1:], lambda c: (c, 0, 0, 0))],
        out_specs=pl.BlockSpec((chunk_len, GROUP, head_dim), lambda c: (0, c, 0)),
        compiler_params=pltpu.CompilerParams(vmem_limit_bytes=48 << 20),
        name='attention',
    )(q, kv, new)


def by_chunk(k, v):
    n, t, h, d = k.shape
    both = jnp.stack([k, v], axis=1).reshape(n, 2, t, N_CH, h // N_CH, d)
    return both.transpose(0, 3, 1, 4, 2, 5).reshape(n, N_CH, 2 * h // N_CH, t, d)


def solution(mesh):
    n_dev = mesh.shape['pool']

    def padded_exchange(k_pool, v_pool, block_table):
        per_dev = k_pool.shape[0]
        n_pref = block_table.shape[1]
        my_index = lax.axis_index('pool')
        pair_cap = 2
        owners = block_table // per_dev
        owned_here = (owners == my_index).astype(jnp.int32)
        send_slot = jnp.where(owned_here > 0, jnp.cumsum(owned_here, axis=1) - 1, pair_cap)
        dest_dev = jnp.broadcast_to(jnp.arange(n_dev)[:, None], send_slot.shape)
        send_ids = jnp.zeros((n_dev, pair_cap), jnp.int32).at[dest_dev, send_slot].set(block_table % per_dev, mode='drop')
        k_recv = lax.all_to_all(k_pool[send_ids], 'pool', 0, 0, tiled=True)
        v_recv = lax.all_to_all(v_pool[send_ids], 'pool', 0, 0, tiled=True)
        my_owners = lax.dynamic_slice_in_dim(owners, my_index, 1, 0).reshape(-1)
        from_owner = (my_owners[:, None] == jnp.arange(n_dev)[None, :]).astype(jnp.int32)
        slot_rank = jnp.sum(from_owner * (jnp.cumsum(from_owner, axis=0) - 1), axis=1)
        recv_idx = my_owners * pair_cap + slot_rank
        flat = (n_dev * pair_cap,) + k_pool.shape[1:]
        pairs = by_chunk(k_recv.reshape(flat)[recv_idx], v_recv.reshape(flat)[recv_idx])
        parts, t, d = pairs.shape[2:]
        pairs = pairs.reshape(n_pref // PAIR_CAP, PAIR_CAP, N_CH, parts, t, d).transpose(2, 0, 3, 1, 4, 5)
        return pairs.reshape(N_CH, n_pref // PAIR_CAP, parts, PAIR_CAP * t, d)

    def local_step(queries, k_new, v_new, k_pool, v_pool, block_table, write_ids):
        block_len = k_pool.shape[1]
        new_shape = (queries.shape[1] // block_len, block_len) + k_new.shape[2:]
        k_blocks, v_blocks = k_new.reshape(new_shape), v_new.reshape(new_shape)
        k_pool_out, v_pool_out, fits, first, second, zsend = prepare(write_ids, block_table.T, k_pool, v_pool, k_blocks, v_blocks)
        attn_out = lax.cond(
            fits[0, 0] > 0,
            lambda: exchange_attention(first, second, queries[0], zsend, k_blocks, v_blocks),
            lambda: attention(queries[0], padded_exchange(k_pool, v_pool, block_table), by_chunk(k_new, v_new)[0]))[None]
        return attn_out, k_pool_out, v_pool_out

    row_spec = P('pool')
    return jax.shard_map(local_step, mesh=mesh, in_specs=(row_spec, row_spec, row_spec, row_spec, row_spec, P(), row_spec), out_specs=(row_spec, row_spec, row_spec), check_vma=False)
```

```python
import functools

import jax
import jax.numpy as jnp
from jax import lax
from jax.experimental import pallas as pl
from jax.experimental.pallas import tpu as pltpu
from jax.sharding import PartitionSpec as P

MESH = pl.DeviceIdType.MESH
PLANES = 4
PLANE = 32
Z_CAP = 10
PAIR_CAP = 2
N_CH = 8
GROUP = 8
TILE = 32
LOG2E = 1.4426950408889634
RING = 4
GROUP_CAP = 10
LAG = 3
STEPS = (1, 3, 2)


def attend_head(q_ref, kv, new, out_ref, ch):
    chunk_len, head_dim = q_ref.shape[0], q_ref.shape[2]
    scale = head_dim ** -0.5 * LOG2E
    heads = pl.ds(ch * GROUP, GROUP)
    k_pref, v_pref = kv(0), kv(1)
    k_new, v_new = new(0), new(1)

    def scores(t):
        q = q_ref[pl.ds(t * TILE, TILE), heads, :].astype(jnp.float32).reshape(TILE * GROUP, head_dim).astype(jnp.bfloat16)
        return nt(q, k_pref), nt(q, k_new)

    n_tile = chunk_len // TILE
    ahead = scores(0)
    for t in range(n_tile):
        s_pref, s_self = ahead
        if t + 1 < n_tile:
            ahead = scores(t + 1)
        token = t * TILE + lax.broadcasted_iota(jnp.int32, s_self.shape, 0) // GROUP
        s_self = jnp.where(token >= lax.broadcasted_iota(jnp.int32, s_self.shape, 1), s_self, -jnp.inf)
        top = jnp.maximum(jnp.max(s_pref, axis=1, keepdims=True), jnp.max(s_self, axis=1, keepdims=True))
        e_pref = jnp.exp2((s_pref - top) * scale)
        e_self = jnp.exp2((s_self - top) * scale)
        inv = 1.0 / (jnp.sum(e_pref, axis=1, keepdims=True) + jnp.sum(e_self, axis=1, keepdims=True))
        p_pref = (e_pref * inv).astype(jnp.bfloat16)
        p_self = (e_self * inv).astype(jnp.bfloat16)
        acc = jnp.dot(p_pref, v_pref, preferred_element_type=jnp.float32) + jnp.dot(p_self, v_new, preferred_element_type=jnp.float32)
        out_ref[pl.ds(t * TILE, TILE), heads, :] = acc.reshape(TILE, GROUP, head_dim).astype(jnp.bfloat16)


def head_major(src, wide, store, blocks):
    for i in range(blocks):
        tokens, heads, dim = wide.shape[1:]
        slot = i % wide.shape[0]
        wide[slot] = src(i).astype(jnp.float32)
        flat = wide.at[slot].reshape(tokens * heads, dim)
        for h in range(heads):
            store(i, h, flat[pl.ds(h, tokens, stride=heads), :].astype(jnp.bfloat16))


def iota(shape, dim):
    return lax.broadcasted_iota(jnp.int32, shape, dim)


def flag(mask):
    return jnp.where(mask, 1.0, 0.0).astype(jnp.bfloat16)


def nt(a, b):
    return lax.dot_general(a, b, (((1,), (1,)), ((), ())), preferred_element_type=jnp.float32)


class Table:
    def __init__(self, table, per_dev):
        owner = table // per_dev
        self.per_dev, self.n_key, self.n_row = per_dev, PLANES * per_dev, table.shape[1]
        self.col = owner % PLANE
        self.key = owner // PLANE * per_dev + table % per_dev

    def hots(self, q):
        match = self.col == q
        ends = (jnp.min(jnp.where(match, self.key, self.n_key - 1), axis=0, keepdims=True), jnp.max(jnp.where(match, self.key, 0), axis=0, keepdims=True))
        return [flag(iota((self.n_key, self.n_row), 0) == end) for end in ends]

    def slots(self, q):
        first, last = self.hots(q)
        every = flag(iota((8, self.n_row), 0) >= 0)
        named = jnp.where(nt(every, first) + nt(every, last) > 0, 1.0, 0.0)
        i, j = iota((self.n_key, self.n_key), 0), iota((self.n_key, self.n_key), 1)
        before = flag((i < j) & (i // self.per_dev == j // self.per_dev))
        rank = jnp.dot(named.astype(jnp.bfloat16), before, preferred_element_type=jnp.float32)
        return named[:1], rank[:1]


def prepare_kernel(wid_ref, table_hbm, k_pool_hbm, v_pool_hbm, k_new_hbm, v_new_hbm, k_out_hbm, v_out_hbm, zsend_ref,
                   table_ref, k_pool, v_pool, k_new, v_new, idx_vec, idx_smem, wide, in_sem, out_sem, idx_sem):
    me = lax.axis_index('pool')
    my_z, my_pos = me // PLANE, lax.rem(me, PLANE)
    per_dev = k_pool.shape[0]
    get_table = pltpu.make_async_copy(table_hbm, table_ref, idx_sem)
    get_table.start()
    loads = [pltpu.make_async_copy(src, dst, in_sem.at[i]) for i, (src, dst) in enumerate(
        ((k_pool_hbm, k_pool), (v_pool_hbm, v_pool), (k_new_hbm, k_new), (v_new_hbm, v_new)))]
    for copy in loads:
        copy.start()
    get_table.wait()
    table = Table(table_ref[...], per_dev)
    named, rank = table.slots(my_pos)
    key = iota((16, table.n_key), 1)
    hit = (named > 0) & (rank == iota((16, table.n_key), 0).astype(jnp.float32)) & (key // per_dev == my_z)
    chosen = jnp.sum(jnp.where(hit, key % per_dev, 0), axis=1, keepdims=True)
    idx_vec[...] = jnp.broadcast_to(chosen, idx_vec.shape)
    to_smem = pltpu.make_async_copy(idx_vec, idx_smem, idx_sem)
    to_smem.start()

    for copy in loads:
        copy.wait()
    pools = [pltpu.make_async_copy(src, dst, out_sem.at[i]) for i, (src, dst) in enumerate(((k_pool, k_out_hbm), (v_pool, v_out_hbm)))]
    for copy in pools:
        copy.start()
    to_smem.wait()

    def send_blocks(part, pool):
        def store(i, h, x):
            zsend_ref[h, i, part] = x
        head_major(lambda i: pool[idx_smem[i, 0]], wide, store, Z_CAP)

    send_blocks(0, k_pool)
    for copy in pools:
        copy.wait()
    writes = []
    for i in range(k_new.shape[0]):
        for part, (src, dst) in enumerate(((k_new, k_out_hbm), (v_new, v_out_hbm))):
            writes.append(pltpu.make_async_copy(src.at[i], dst.at[wid_ref[0, i]], in_sem.at[2 * i + part]))
            writes[-1].start()
    send_blocks(1, v_pool)
    for copy in writes:
        copy.wait()


def prepare(write_ids, table_t, k_pool, v_pool, k_new, v_new):
    tokens, heads, dim = k_pool.shape[1:]
    vmem, smem, hbm = (pl.BlockSpec(memory_space=m) for m in (pltpu.VMEM, pltpu.SMEM, pl.ANY))
    return pl.pallas_call(
        prepare_kernel,
        out_shape=[jax.ShapeDtypeStruct(k_pool.shape, k_pool.dtype), jax.ShapeDtypeStruct(v_pool.shape, v_pool.dtype),
                   jax.ShapeDtypeStruct((N_CH, Z_CAP, 2, tokens, dim), k_pool.dtype)],
        in_specs=[smem, hbm, hbm, hbm, hbm, hbm],
        out_specs=[hbm, hbm, vmem],
        scratch_shapes=[pltpu.VMEM(table_t.shape, jnp.int32), pltpu.VMEM(k_pool.shape, k_pool.dtype), pltpu.VMEM(k_pool.shape, k_pool.dtype),
                        pltpu.VMEM(k_new.shape, k_pool.dtype), pltpu.VMEM(k_new.shape, k_pool.dtype),
                        pltpu.VMEM((16, 128), jnp.int32), pltpu.SMEM((16, 128), jnp.int32), pltpu.VMEM((4, tokens, heads, dim), jnp.float32),
                        pltpu.SemaphoreType.DMA((2 * k_new.shape[0],)), pltpu.SemaphoreType.DMA((2,)), pltpu.SemaphoreType.DMA],
        compiler_params=pltpu.CompilerParams(vmem_limit_bytes=32 << 20),
        name='prepare',
    )(write_ids, table_t, k_pool, v_pool, k_new, v_new)


def members(n_group, n_row, plane_of):
    group, row = iota((n_group, n_row), 0), iota((n_group, n_row), 1)
    at = jnp.where(group // RING % 2 == 0, row // 8 % RING, row // 2 % RING)
    return flag((row // PLANE == plane_of(group)) & (at == group % RING))


def capacity_check(table, named_by_column):
    groups = members(2 * RING * PLANES, table.n_row, lambda g: g // (2 * RING))
    n_group = groups.shape[0]

    def widest(q, most):
        first, last = table.hots(q)
        named = jnp.where(nt(groups, first) + nt(groups, last) > 0, 1.0, 0.0)
        named_by_column[pl.ds(q, 1), :] = jnp.max(named, axis=0, keepdims=True)
        return jnp.maximum(most, jnp.sum(named, axis=1, keepdims=True))

    most_in_group = lax.fori_loop(0, PLANE, widest, jnp.zeros((n_group, 1), jnp.float32), unroll=4)
    per_plane = flag(iota((table.n_key, 128), 0) // table.per_dev == iota((table.n_key, 128), 1))
    by_device = jnp.dot(named_by_column[...].astype(jnp.bfloat16), per_plane, preferred_element_type=jnp.float32)
    in_col = jnp.zeros((1, table.n_row), jnp.int32)
    for q in range(PLANE):
        in_col = jnp.maximum(in_col, jnp.sum(jnp.where(table.col == q, 1, 0), axis=0, keepdims=True))

    def top(a):
        return jnp.max(jnp.max(a, axis=1, keepdims=True), axis=0, keepdims=True)

    return jnp.where((top(in_col) <= PAIR_CAP) & (top(by_device) <= Z_CAP) & (top(most_in_group) <= GROUP_CAP), 1, 0)


def routing(table, my_z, my_y, my_x, my_c, first_ref, second_ref):
    n_key, n_row = table.n_key, table.n_row
    my_pos = my_y * 8 + my_x * 2 + my_c
    _, rank = table.slots(my_pos)
    slot_row = jnp.minimum(rank, Z_CAP - 1.0) + (iota(rank.shape, 1) // table.per_dev * Z_CAP).astype(jnp.float32)
    groups = members(2 * RING, n_row, lambda g: my_z)
    before = flag(iota((n_key, n_key), 0) < iota((n_key, n_key), 1))

    def lists(q):
        hots = table.hots(q)
        listed = jnp.where(nt(groups, hots[0]) + nt(groups, hots[1]) > 0, 1.0, 0.0)
        return hots, listed, jnp.dot(listed.astype(jnp.bfloat16), before, preferred_element_type=jnp.float32)

    _, listed, place = lists(my_pos)
    first_step = jnp.zeros((2 * RING, 128), jnp.int32)
    for i in range(GROUP_CAP):
        at = jnp.sum(jnp.where((listed > 0) & (place == i), slot_row, 0.0), axis=1, keepdims=True).astype(jnp.int32)
        first_step = jnp.where(iota(first_step.shape, 1) == i, at, first_step)
    first_ref[...] = jnp.clip(first_step, 0, PLANES * Z_CAP - 1)
    for part in range(2):
        for src in range(RING):
            q = (src * 8 + my_x * 2 + my_c) if part == 0 else (my_y * 8 + src * 2 + my_c)
            mine_at = my_y if part == 0 else RING + my_x
            hots, _, place = lists(q)
            for end in range(PAIR_CAP):
                found = jnp.dot(place.astype(jnp.bfloat16), hots[end], preferred_element_type=jnp.float32)
                found = jnp.sum(jnp.where(iota(found.shape, 0) == mine_at, found, 0.0), axis=0, keepdims=True)
                line = (part * RING + src) * PAIR_CAP + end
                second_ref[line:line + 1, :] = jnp.clip(found.astype(jnp.int32), 0, GROUP_CAP - 1) + src * GROUP_CAP


def exchange_kernel(per_dev, table_hbm, q_hbm, zsend_hbm, k_new_hbm, v_new_hbm, out_hbm, fits_hbm, q_ref, out_ref, recv_k, recv_v, k_new, v_new,
                    new_t, wide, zsend, table_ref, first_vec, second_vec, first_ref, second_ref, named_by_column, fits_vec, *scratch):
    zrecv, send1, recv1, send2 = (scratch[:N_CH], scratch[N_CH:3 * N_CH], scratch[3 * N_CH:5 * N_CH], scratch[5 * N_CH:7 * N_CH])
    zs_sem, zr_sem, s1_sem, r1_sem, s2_sem, r2_sem, in_sem, out_sem = scratch[7 * N_CH:]
    me = lax.axis_index('pool')
    my_z, my_pos = me // PLANE, lax.rem(me, PLANE)
    base = my_z * PLANE
    y, x, c = my_pos // 8, lax.rem(my_pos // 2, RING), lax.rem(my_pos, 2)
    head_dim = q_ref.shape[2]

    def z_peer(d):
        return lax.rem(my_z + d, PLANES) * PLANE + my_pos

    def y_peer(d, dc):
        return base + lax.rem(y + d, RING) * 8 + x * 2 + lax.rem(c + dc, 2)

    def x_peer(d, dc):
        return base + y * 8 + lax.rem(x + d, RING) * 2 + lax.rem(c + dc, 2)

    barrier = pltpu.get_barrier_semaphore()
    peers = [z_peer(d) for d in STEPS] + [peer(d, dc) for d in STEPS for dc in range(2) for peer in (y_peer, x_peer)] + [y_peer(0, 1)]
    for peer in peers:
        pl.semaphore_signal(barrier, inc=1, device_id=(peer,), device_id_type=MESH)

    loads = [pltpu.make_async_copy(src, dst, in_sem.at[i]) for i, (src, dst) in enumerate(
        ((zsend_hbm, zsend), (k_new_hbm, k_new), (v_new_hbm, v_new), (q_hbm, q_ref), (table_hbm, table_ref)))]
    to_smem = [pltpu.make_async_copy(src, dst, in_sem.at[5 + i]) for i, (src, dst) in enumerate(((first_vec, first_ref), (second_vec, second_ref)))]
    fits_copy = pltpu.make_async_copy(fits_vec, fits_hbm, in_sem.at[7])
    for copy in loads:
        copy.start()

    def remote(src, dst, send_sem, recv_sem, peer):
        return pltpu.make_async_remote_copy(
            src_ref=src, dst_ref=dst, send_sem=send_sem, recv_sem=recv_sem, device_id=(peer,), device_id_type=MESH)

    def wait_bytes(ref, sem):
        pltpu.make_async_copy(ref, ref, sem).wait()

    def z_wait(ch, sem):
        wait_bytes(zrecv[ch].at[pl.ds(0, (PLANES - 1) * Z_CAP)], sem.at[ch])

    def wait1(i, sem):
        wait_bytes(recv1[i].at[pl.ds(0, (RING - 1) * GROUP_CAP)], sem.at[i])

    def wait2(i, sem):
        wait_bytes(send2[i].at[pl.ds(0, 2 * RING - 1)], sem.at[i])

    def step1(ch):
        for part in range(2):
            i = 2 * ch + part
            for g in range(RING):
                for s in range(GROUP_CAP):
                    send1[i][g, s] = zrecv[ch][first_ref[part * RING + g, s], part]
            mine = y if part == 0 else x
            recv1[i][pl.ds(mine * GROUP_CAP, GROUP_CAP)] = send1[i][mine]
        for d in STEPS:
            for part in range(2):
                i = 2 * ch + part
                mine, peer = (y, y_peer(d, 0)) if part == 0 else (x, x_peer(d, 0))
                remote(send1[i].at[lax.rem(mine + d, RING)], recv1[i].at[pl.ds(mine * GROUP_CAP, GROUP_CAP)],
                       s1_sem.at[i], r1_sem.at[i], peer).start()

    def step2(ch):
        for part in range(2):
            i = 2 * ch + part
            wait1(i, r1_sem)

            @pl.loop(0, RING)
            def _(to):
                for core in range(2):
                    row = base + ((y * 8 + to * 2) if part == 0 else (to * 8 + x * 2)) + core
                    for src in range(RING):
                        for end in range(PAIR_CAP):
                            send2[i][to * 2 + core, src, end * 16:(end + 1) * 16, :] = recv1[i][second_ref[(part * RING + src) * PAIR_CAP + end, row]]

        recv_k[ch, :, x, c] = send2[2 * ch][x * 2 + c]
        recv_v[ch, y, :, c] = send2[2 * ch + 1][y * 2 + c]
        for d in STEPS + (0,):
            for dc in range(2):
                for part in range(2):
                    if (d, dc) == (0, 0):
                        continue
                    i = 2 * ch + part
                    mine, peer = (x, x_peer(d, dc)) if part == 0 else (y, y_peer(d, dc))
                    dst = recv_k.at[ch, :, x, c] if part == 0 else recv_v.at[ch, y, :, c]
                    remote(send2[i].at[lax.rem(mine + d, RING) * 2 + lax.rem(c + dc, 2)], dst, s2_sem.at[i], r2_sem.at[i], peer).start()

    def out_copy(ch):
        heads = pl.ds(ch * GROUP, GROUP)
        return pltpu.make_async_copy(out_ref.at[:, heads, :], out_hbm.at[:, heads, :], out_sem.at[ch])

    def attend(ch):
        wait2(2 * ch, r2_sem)
        wait2(2 * ch + 1, r2_sem)
        recv = (recv_k, recv_v)
        attend_head(q_ref, lambda part: recv[part][ch].reshape(-1, head_dim), lambda part: new_t[ch, part], out_ref, ch)
        out_copy(ch).start()

    loads[0].wait()
    pl.semaphore_wait(barrier, len(peers))
    for ch in range(N_CH):
        for d in STEPS:
            remote(zsend.at[ch], zrecv[ch].at[pl.ds(my_z * Z_CAP, Z_CAP)], zs_sem.at[ch], zr_sem.at[ch], z_peer(d)).start()
    loads[4].wait()
    table = Table(table_ref[...], per_dev)
    routing(table, my_z, y, x, c, first_vec, second_vec)
    for copy in to_smem:
        copy.start()
    for ch in range(N_CH):
        zrecv[ch][pl.ds(my_z * Z_CAP, Z_CAP)] = zsend[ch]
    for copy in to_smem:
        copy.wait()

    def new_keys():
        for part, block in enumerate((k_new, v_new)):
            loads[1 + part].wait()

            def store(i, h, x):
                new_t[h, part, i * 16:(i + 1) * 16, :] = x
            head_major(lambda i: block[i], wide, store, block.shape[0])
        loads[3].wait()

    for t in range(N_CH + LAG):
        if t < N_CH:
            z_wait(t, zr_sem)
            step1(t)
        if t == 0:
            new_keys()
        if t == 1:
            fits_vec[...] = jnp.broadcast_to(capacity_check(table, named_by_column), fits_vec.shape)
            fits_copy.start()
        if 1 <= t <= N_CH:
            step2(t - 1)
        if t >= LAG:
            attend(t - LAG)
    fits_copy.wait()
    for ch in range(N_CH):
        z_wait(ch, zs_sem)
        out_copy(ch).wait()
    for i in range(2 * N_CH):
        wait1(i, s1_sem)
        wait2(i, s2_sem)


def exchange_attention(table_t, q, zsend, k_new, v_new, per_dev):
    tokens, dim = zsend.shape[3:]
    dtype = q.dtype
    hbm = pl.BlockSpec(memory_space=pl.ANY)
    recv = pltpu.VMEM((N_CH, RING, RING, 2, PAIR_CAP * tokens, dim), dtype)
    tables = [(2 * RING, 128), (2 * RING * PAIR_CAP, table_t.shape[1])]
    return pl.pallas_call(
        functools.partial(exchange_kernel, per_dev),
        out_shape=[jax.ShapeDtypeStruct(q.shape, dtype), jax.ShapeDtypeStruct((8, 128), jnp.int32)],
        in_specs=[hbm] * 5,
        out_specs=[hbm, hbm],
        scratch_shapes=[pltpu.VMEM(q.shape, dtype), pltpu.VMEM(q.shape, dtype), recv, recv,
                        pltpu.VMEM(k_new.shape, dtype), pltpu.VMEM(v_new.shape, dtype), pltpu.VMEM((N_CH, 2, q.shape[0], q.shape[2]), dtype),
                        pltpu.VMEM((4,) + k_new.shape[1:], jnp.float32), pltpu.VMEM(zsend.shape, dtype), pltpu.VMEM(table_t.shape, jnp.int32)]
        + [pltpu.VMEM(shape, jnp.int32) for shape in tables] + [pltpu.SMEM(shape, jnp.int32) for shape in tables]
        + [pltpu.VMEM((PLANE, 128), jnp.float32), pltpu.VMEM((8, 128), jnp.int32)]
        + [pltpu.VMEM((PLANES * Z_CAP, 2, tokens, dim), dtype)] * N_CH
        + [pltpu.VMEM((RING, GROUP_CAP, tokens, dim), dtype)] * (2 * N_CH)
        + [pltpu.VMEM((RING * GROUP_CAP, tokens, dim), dtype)] * (2 * N_CH)
        + [pltpu.VMEM((2 * RING, RING, PAIR_CAP * tokens, dim), dtype)] * (2 * N_CH)
        + [pltpu.SemaphoreType.DMA((N_CH,))] * 2 + [pltpu.SemaphoreType.DMA((2 * N_CH,))] * 4 + [pltpu.SemaphoreType.DMA((N_CH,))] * 2,
        compiler_params=pltpu.CompilerParams(collective_id=0, has_side_effects=True, vmem_limit_bytes=56 << 20),
        name='exchange_attention',
    )(table_t, q, zsend, k_new, v_new)


def attention_kernel(q_ref, kv_ref, new_ref, out_ref):
    head_dim = q_ref.shape[2]
    attend_head(q_ref, lambda part: kv_ref[0, :, part].reshape(-1, head_dim), lambda part: new_ref[0, part], out_ref, 0)


def attention(q, kv, new):
    chunk_len, q_heads, head_dim = q.shape
    return pl.pallas_call(
        attention_kernel,
        grid=(N_CH,),
        out_shape=jax.ShapeDtypeStruct(q.shape, q.dtype),
        in_specs=[pl.BlockSpec((chunk_len, GROUP, head_dim), lambda c: (0, c, 0)),
                  pl.BlockSpec((1,) + kv.shape[1:], lambda c: (c, 0, 0, 0, 0)),
                  pl.BlockSpec((1,) + new.shape[1:], lambda c: (c, 0, 0, 0))],
        out_specs=pl.BlockSpec((chunk_len, GROUP, head_dim), lambda c: (0, c, 0)),
        compiler_params=pltpu.CompilerParams(vmem_limit_bytes=48 << 20),
        name='attention',
    )(q, kv, new)


def by_chunk(k, v):
    n, t, h, d = k.shape
    both = jnp.stack([k, v], axis=1).reshape(n, 2, t, N_CH, h // N_CH, d)
    return both.transpose(0, 3, 1, 4, 2, 5).reshape(n, N_CH, 2 * h // N_CH, t, d)


def solution(mesh):
    n_dev = mesh.shape['pool']

    def padded_exchange(k_pool, v_pool, block_table):
        per_dev = k_pool.shape[0]
        n_pref = block_table.shape[1]
        my_index = lax.axis_index('pool')
        pair_cap = 2
        owners = block_table // per_dev
        owned_here = (owners == my_index).astype(jnp.int32)
        send_slot = jnp.where(owned_here > 0, jnp.cumsum(owned_here, axis=1) - 1, pair_cap)
        dest_dev = jnp.broadcast_to(jnp.arange(n_dev)[:, None], send_slot.shape)
        send_ids = jnp.zeros((n_dev, pair_cap), jnp.int32).at[dest_dev, send_slot].set(block_table % per_dev, mode='drop')
        k_recv = lax.all_to_all(k_pool[send_ids], 'pool', 0, 0, tiled=True)
        v_recv = lax.all_to_all(v_pool[send_ids], 'pool', 0, 0, tiled=True)
        my_owners = lax.dynamic_slice_in_dim(owners, my_index, 1, 0).reshape(-1)
        from_owner = (my_owners[:, None] == jnp.arange(n_dev)[None, :]).astype(jnp.int32)
        slot_rank = jnp.sum(from_owner * (jnp.cumsum(from_owner, axis=0) - 1), axis=1)
        recv_idx = my_owners * pair_cap + slot_rank
        flat = (n_dev * pair_cap,) + k_pool.shape[1:]
        pairs = by_chunk(k_recv.reshape(flat)[recv_idx], v_recv.reshape(flat)[recv_idx])
        parts, t, d = pairs.shape[2:]
        pairs = pairs.reshape(n_pref // PAIR_CAP, PAIR_CAP, N_CH, parts, t, d).transpose(2, 0, 3, 1, 4, 5)
        return pairs.reshape(N_CH, n_pref // PAIR_CAP, parts, PAIR_CAP * t, d)

    def local_step(queries, k_new, v_new, k_pool, v_pool, block_table, write_ids):
        block_len = k_pool.shape[1]
        new_shape = (queries.shape[1] // block_len, block_len) + k_new.shape[2:]
        k_blocks, v_blocks = k_new.reshape(new_shape), v_new.reshape(new_shape)
        k_pool_out, v_pool_out, zsend = prepare(write_ids, block_table.T, k_pool, v_pool, k_blocks, v_blocks)
        fast, fits = exchange_attention(block_table.T, queries[0], zsend, k_blocks, v_blocks, k_pool.shape[0])
        attn_out = lax.cond(
            fits[0, 0] > 0,
            lambda: fast,
            lambda: attention(queries[0], padded_exchange(k_pool, v_pool, block_table), by_chunk(k_new, v_new)[0]))[None]
        return attn_out, k_pool_out, v_pool_out

    row_spec = P('pool')
    return jax.shard_map(local_step, mesh=mesh, in_specs=(row_spec, row_spec, row_spec, row_spec, row_spec, P(), row_spec), out_specs=(row_spec, row_spec, row_spec), check_vma=False)
```

```python
import functools

import jax
import jax.numpy as jnp
from jax import lax
from jax.experimental import pallas as pl
from jax.experimental.pallas import tpu as pltpu
from jax.sharding import PartitionSpec as P

MESH = pl.DeviceIdType.MESH
PLANES = 4
PLANE = 32
Z_CAP = 10
PAIR_CAP = 2
N_CH = 8
GROUP = 8
TILE = 32
LOG2E = 1.4426950408889634
RING = 4
GROUP_CAP = 10
LAG = 3
STEPS = (1, 3, 2)


def attend_head(q_ref, kv, new, out_ref, ch):
    chunk_len, head_dim = q_ref.shape[0], q_ref.shape[2]
    scale = head_dim ** -0.5 * LOG2E
    heads = pl.ds(ch * GROUP, GROUP)
    k_pref, v_pref = kv(0), kv(1)
    k_new, v_new = new(0), new(1)

    def scores(t):
        q = q_ref[pl.ds(t * TILE, TILE), heads, :].astype(jnp.float32).reshape(TILE * GROUP, head_dim).astype(jnp.bfloat16)
        return nt(q, k_pref), nt(q, k_new)

    n_tile = chunk_len // TILE
    ahead = scores(0)
    for t in range(n_tile):
        s_pref, s_self = ahead
        if t + 1 < n_tile:
            ahead = scores(t + 1)
        token = t * TILE + lax.broadcasted_iota(jnp.int32, s_self.shape, 0) // GROUP
        s_self = jnp.where(token >= lax.broadcasted_iota(jnp.int32, s_self.shape, 1), s_self, -jnp.inf)
        top = jnp.maximum(jnp.max(s_pref, axis=1, keepdims=True), jnp.max(s_self, axis=1, keepdims=True))
        e_pref = jnp.exp2((s_pref - top) * scale)
        e_self = jnp.exp2((s_self - top) * scale)
        inv = 1.0 / (jnp.sum(e_pref, axis=1, keepdims=True) + jnp.sum(e_self, axis=1, keepdims=True))
        p_pref = (e_pref * inv).astype(jnp.bfloat16)
        p_self = (e_self * inv).astype(jnp.bfloat16)
        acc = jnp.dot(p_pref, v_pref, preferred_element_type=jnp.float32) + jnp.dot(p_self, v_new, preferred_element_type=jnp.float32)
        out_ref[pl.ds(t * TILE, TILE), heads, :] = acc.reshape(TILE, GROUP, head_dim).astype(jnp.bfloat16)


def head_major(src, wide, store, blocks):
    for i in range(blocks):
        tokens, heads, dim = wide.shape[1:]
        slot = i % wide.shape[0]
        wide[slot] = src(i).astype(jnp.float32)
        flat = wide.at[slot].reshape(tokens * heads, dim)
        for h in range(heads):
            store(i, h, flat[pl.ds(h, tokens, stride=heads), :].astype(jnp.bfloat16))


def iota(shape, dim):
    return lax.broadcasted_iota(jnp.int32, shape, dim)


def flag(mask):
    return jnp.where(mask, 1.0, 0.0).astype(jnp.bfloat16)


def nt(a, b):
    return lax.dot_general(a, b, (((1,), (1,)), ((), ())), preferred_element_type=jnp.float32)


class Table:
    def __init__(self, table, per_dev):
        owner = table // per_dev
        self.per_dev, self.n_key, self.n_row = per_dev, PLANES * per_dev, table.shape[1]
        self.col = owner % PLANE
        self.key = owner // PLANE * per_dev + table % per_dev

    def hots(self, q):
        match = self.col == q
        ends = (jnp.min(jnp.where(match, self.key, self.n_key - 1), axis=0, keepdims=True), jnp.max(jnp.where(match, self.key, 0), axis=0, keepdims=True))
        return [flag(iota((self.n_key, self.n_row), 0) == end) for end in ends]

    def slots(self, q):
        first, last = self.hots(q)
        every = flag(iota((8, self.n_row), 0) >= 0)
        named = jnp.where(nt(every, first) + nt(every, last) > 0, 1.0, 0.0)
        i, j = iota((self.n_key, self.n_key), 0), iota((self.n_key, self.n_key), 1)
        before = flag((i < j) & (i // self.per_dev == j // self.per_dev))
        rank = jnp.dot(named.astype(jnp.bfloat16), before, preferred_element_type=jnp.float32)
        return named[:1], rank[:1]


def prepare_kernel(wid_ref, table_hbm, k_pool_hbm, v_pool_hbm, k_new_hbm, v_new_hbm, k_out_hbm, v_out_hbm, zsend_ref,
                   table_ref, k_pool, v_pool, k_new, v_new, idx_vec, idx_smem, wide, in_sem, out_sem, idx_sem):
    me = lax.axis_index('pool')
    my_z, my_pos = me // PLANE, lax.rem(me, PLANE)
    per_dev = k_pool.shape[0]
    get_table = pltpu.make_async_copy(table_hbm, table_ref, idx_sem)
    get_table.start()
    loads = [pltpu.make_async_copy(src, dst, in_sem.at[i]) for i, (src, dst) in enumerate(
        ((k_pool_hbm, k_pool), (v_pool_hbm, v_pool), (k_new_hbm, k_new), (v_new_hbm, v_new)))]
    for copy in loads:
        copy.start()
    get_table.wait()
    table = Table(table_ref[...], per_dev)
    named, rank = table.slots(my_pos)
    key = iota((16, table.n_key), 1)
    hit = (named > 0) & (rank == iota((16, table.n_key), 0).astype(jnp.float32)) & (key // per_dev == my_z)
    chosen = jnp.sum(jnp.where(hit, key % per_dev, 0), axis=1, keepdims=True)
    idx_vec[...] = jnp.broadcast_to(chosen, idx_vec.shape)
    to_smem = pltpu.make_async_copy(idx_vec, idx_smem, idx_sem)
    to_smem.start()

    for copy in loads:
        copy.wait()
    pools = [pltpu.make_async_copy(src, dst, out_sem.at[i]) for i, (src, dst) in enumerate(((k_pool, k_out_hbm), (v_pool, v_out_hbm)))]
    for copy in pools:
        copy.start()
    to_smem.wait()

    def send_blocks(part, pool):
        def store(i, h, x):
            zsend_ref[h, i, part] = x
        head_major(lambda i: pool[idx_smem[i, 0]], wide, store, Z_CAP)

    send_blocks(0, k_pool)
    for copy in pools:
        copy.wait()
    writes = []
    for i in range(k_new.shape[0]):
        for part, (src, dst) in enumerate(((k_new, k_out_hbm), (v_new, v_out_hbm))):
            writes.append(pltpu.make_async_copy(src.at[i], dst.at[wid_ref[0, i]], in_sem.at[2 * i + part]))
            writes[-1].start()
    send_blocks(1, v_pool)
    for copy in writes:
        copy.wait()


def prepare(write_ids, table_t, k_pool, v_pool, k_new, v_new):
    tokens, heads, dim = k_pool.shape[1:]
    vmem, smem, hbm = (pl.BlockSpec(memory_space=m) for m in (pltpu.VMEM, pltpu.SMEM, pl.ANY))
    return pl.pallas_call(
        prepare_kernel,
        out_shape=[jax.ShapeDtypeStruct(k_pool.shape, k_pool.dtype), jax.ShapeDtypeStruct(v_pool.shape, v_pool.dtype),
                   jax.ShapeDtypeStruct((N_CH, Z_CAP, 2, tokens, dim), k_pool.dtype)],
        in_specs=[smem, hbm, hbm, hbm, hbm, hbm],
        out_specs=[hbm, hbm, vmem],
        scratch_shapes=[pltpu.VMEM(table_t.shape, jnp.int32), pltpu.VMEM(k_pool.shape, k_pool.dtype), pltpu.VMEM(k_pool.shape, k_pool.dtype),
                        pltpu.VMEM(k_new.shape, k_pool.dtype), pltpu.VMEM(k_new.shape, k_pool.dtype),
                        pltpu.VMEM((16, 128), jnp.int32), pltpu.SMEM((16, 128), jnp.int32), pltpu.VMEM((4, tokens, heads, dim), jnp.float32),
                        pltpu.SemaphoreType.DMA((2 * k_new.shape[0],)), pltpu.SemaphoreType.DMA((2,)), pltpu.SemaphoreType.DMA],
        compiler_params=pltpu.CompilerParams(vmem_limit_bytes=32 << 20),
        name='prepare',
    )(write_ids, table_t, k_pool, v_pool, k_new, v_new)


def members(n_group, n_row, plane_of):
    group, row = iota((n_group, n_row), 0), iota((n_group, n_row), 1)
    at = jnp.where(group // RING % 2 == 0, row // 8 % RING, row // 2 % RING)
    return flag((row // PLANE == plane_of(group)) & (at == group % RING))


def capacity_check(table, named_by_column):
    groups = members(2 * RING * PLANES, table.n_row, lambda g: g // (2 * RING))
    n_group = groups.shape[0]

    def widest(q, most):
        first, last = table.hots(q)
        named = jnp.where(nt(groups, first) + nt(groups, last) > 0, 1.0, 0.0)
        named_by_column[pl.ds(q, 1), :] = jnp.max(named, axis=0, keepdims=True)
        return jnp.maximum(most, jnp.sum(named, axis=1, keepdims=True))

    most_in_group = lax.fori_loop(0, PLANE, widest, jnp.zeros((n_group, 1), jnp.float32), unroll=4)
    per_plane = flag(iota((table.n_key, 128), 0) // table.per_dev == iota((table.n_key, 128), 1))
    by_device = jnp.dot(named_by_column[...].astype(jnp.bfloat16), per_plane, preferred_element_type=jnp.float32)
    in_col = jnp.zeros((1, table.n_row), jnp.int32)
    for q in range(PLANE):
        in_col = jnp.maximum(in_col, jnp.sum(jnp.where(table.col == q, 1, 0), axis=0, keepdims=True))

    def top(a):
        return jnp.max(jnp.max(a, axis=1, keepdims=True), axis=0, keepdims=True)

    return jnp.where((top(in_col) <= PAIR_CAP) & (top(by_device) <= Z_CAP) & (top(most_in_group) <= GROUP_CAP), 1, 0)


def routing(table, my_z, my_y, my_x, my_c, first_ref, second_ref):
    n_key, n_row = table.n_key, table.n_row
    my_pos = my_y * 8 + my_x * 2 + my_c
    _, rank = table.slots(my_pos)
    slot_row = jnp.minimum(rank, Z_CAP - 1.0) + (iota(rank.shape, 1) // table.per_dev * Z_CAP).astype(jnp.float32)
    groups = members(2 * RING, n_row, lambda g: my_z)
    before = flag(iota((n_key, n_key), 0) < iota((n_key, n_key), 1))

    def lists(q):
        hots = table.hots(q)
        listed = jnp.where(nt(groups, hots[0]) + nt(groups, hots[1]) > 0, 1.0, 0.0)
        return hots, listed, jnp.dot(listed.astype(jnp.bfloat16), before, preferred_element_type=jnp.float32)

    _, listed, place = lists(my_pos)
    first_step = jnp.zeros((2 * RING, 128), jnp.int32)
    for i in range(GROUP_CAP):
        at = jnp.sum(jnp.where((listed > 0) & (place == i), slot_row, 0.0), axis=1, keepdims=True).astype(jnp.int32)
        first_step = jnp.where(iota(first_step.shape, 1) == i, at, first_step)
    first_ref[...] = jnp.clip(first_step, 0, PLANES * Z_CAP - 1)
    for part in range(2):
        for src in range(RING):
            q = (src * 8 + my_x * 2 + my_c) if part == 0 else (my_y * 8 + src * 2 + my_c)
            mine_at = my_y if part == 0 else RING + my_x
            hots, _, place = lists(q)
            for end in range(PAIR_CAP):
                found = jnp.dot(place.astype(jnp.bfloat16), hots[end], preferred_element_type=jnp.float32)
                found = jnp.sum(jnp.where(iota(found.shape, 0) == mine_at, found, 0.0), axis=0, keepdims=True)
                line = (part * RING + src) * PAIR_CAP + end
                second_ref[line:line + 1, :] = jnp.clip(found.astype(jnp.int32), 0, GROUP_CAP - 1) + src * GROUP_CAP


def exchange_kernel(per_dev, table_hbm, q_hbm, zsend_hbm, k_new_hbm, v_new_hbm, out_ref, fits_hbm, q_ref, recv_k, recv_v, k_new, v_new,
                    new_t, wide, zsend, table_ref, first_vec, second_vec, first_ref, second_ref, named_by_column, fits_vec, *scratch):
    zrecv, send1, recv1, send2 = (scratch[:N_CH], scratch[N_CH:3 * N_CH], scratch[3 * N_CH:5 * N_CH], scratch[5 * N_CH:7 * N_CH])
    zs_sem, zr_sem, s1_sem, r1_sem, s2_sem, r2_sem, in_sem = scratch[7 * N_CH:]
    me = lax.axis_index('pool')
    my_z, my_pos = me // PLANE, lax.rem(me, PLANE)
    base = my_z * PLANE
    y, x, c = my_pos // 8, lax.rem(my_pos // 2, RING), lax.rem(my_pos, 2)
    head_dim = q_ref.shape[2]

    def z_peer(d):
        return lax.rem(my_z + d, PLANES) * PLANE + my_pos

    def y_peer(d, dc):
        return base + lax.rem(y + d, RING) * 8 + x * 2 + lax.rem(c + dc, 2)

    def x_peer(d, dc):
        return base + y * 8 + lax.rem(x + d, RING) * 2 + lax.rem(c + dc, 2)

    barrier = pltpu.get_barrier_semaphore()
    peers = [z_peer(d) for d in STEPS] + [peer(d, dc) for d in STEPS for dc in range(2) for peer in (y_peer, x_peer)] + [y_peer(0, 1)]
    for peer in peers:
        pl.semaphore_signal(barrier, inc=1, device_id=(peer,), device_id_type=MESH)

    loads = [pltpu.make_async_copy(src, dst, in_sem.at[i]) for i, (src, dst) in enumerate(
        ((zsend_hbm, zsend), (k_new_hbm, k_new), (v_new_hbm, v_new), (q_hbm, q_ref), (table_hbm, table_ref)))]
    to_smem = [pltpu.make_async_copy(src, dst, in_sem.at[5 + i]) for i, (src, dst) in enumerate(((first_vec, first_ref), (second_vec, second_ref)))]
    fits_copy = pltpu.make_async_copy(fits_vec, fits_hbm, in_sem.at[7])
    for copy in loads:
        copy.start()

    def remote(src, dst, send_sem, recv_sem, peer):
        return pltpu.make_async_remote_copy(
            src_ref=src, dst_ref=dst, send_sem=send_sem, recv_sem=recv_sem, device_id=(peer,), device_id_type=MESH)

    def wait_bytes(ref, sem):
        pltpu.make_async_copy(ref, ref, sem).wait()

    def z_wait(ch, sem):
        wait_bytes(zrecv[ch].at[pl.ds(0, (PLANES - 1) * Z_CAP)], sem.at[ch])

    def wait1(i, sem):
        wait_bytes(recv1[i].at[pl.ds(0, (RING - 1) * GROUP_CAP)], sem.at[i])

    def wait2(i, sem):
        wait_bytes(send2[i].at[pl.ds(0, 2 * RING - 1)], sem.at[i])

    def step1(ch):
        for part in range(2):
            i = 2 * ch + part
            for g in range(RING):
                for s in range(GROUP_CAP):
                    send1[i][g, s] = zrecv[ch][first_ref[part * RING + g, s], part]
            mine = y if part == 0 else x
            recv1[i][pl.ds(mine * GROUP_CAP, GROUP_CAP)] = send1[i][mine]
        for d in STEPS:
            for part in range(2):
                i = 2 * ch + part
                mine, peer = (y, y_peer(d, 0)) if part == 0 else (x, x_peer(d, 0))
                remote(send1[i].at[lax.rem(mine + d, RING)], recv1[i].at[pl.ds(mine * GROUP_CAP, GROUP_CAP)],
                       s1_sem.at[i], r1_sem.at[i], peer).start()

    def step2(ch):
        for part in range(2):
            i = 2 * ch + part
            wait1(i, r1_sem)

            @pl.loop(0, RING)
            def _(to):
                for core in range(2):
                    row = base + ((y * 8 + to * 2) if part == 0 else (to * 8 + x * 2)) + core
                    for src in range(RING):
                        for end in range(PAIR_CAP):
                            send2[i][to * 2 + core, src, end * 16:(end + 1) * 16, :] = recv1[i][second_ref[(part * RING + src) * PAIR_CAP + end, row]]

        recv_k[ch, :, x, c] = send2[2 * ch][x * 2 + c]
        recv_v[ch, y, :, c] = send2[2 * ch + 1][y * 2 + c]
        for d in STEPS + (0,):
            for dc in range(2):
                for part in range(2):
                    if (d, dc) == (0, 0):
                        continue
                    i = 2 * ch + part
                    mine, peer = (x, x_peer(d, dc)) if part == 0 else (y, y_peer(d, dc))
                    dst = recv_k.at[ch, :, x, c] if part == 0 else recv_v.at[ch, y, :, c]
                    remote(send2[i].at[lax.rem(mine + d, RING) * 2 + lax.rem(c + dc, 2)], dst, s2_sem.at[i], r2_sem.at[i], peer).start()

    def attend(ch):
        wait2(2 * ch, r2_sem)
        wait2(2 * ch + 1, r2_sem)
        recv = (recv_k, recv_v)
        attend_head(q_ref, lambda part: recv[part][ch].reshape(-1, head_dim), lambda part: new_t[ch, part], out_ref, ch)

    loads[0].wait()
    pl.semaphore_wait(barrier, len(peers))
    for ch in range(N_CH):
        for d in STEPS:
            remote(zsend.at[ch], zrecv[ch].at[pl.ds(my_z * Z_CAP, Z_CAP)], zs_sem.at[ch], zr_sem.at[ch], z_peer(d)).start()
    loads[4].wait()
    table = Table(table_ref[...], per_dev)
    routing(table, my_z, y, x, c, first_vec, second_vec)
    for copy in to_smem:
        copy.start()
    for ch in range(N_CH):
        zrecv[ch][pl.ds(my_z * Z_CAP, Z_CAP)] = zsend[ch]
    for copy in to_smem:
        copy.wait()

    def new_keys():
        for part, block in enumerate((k_new, v_new)):
            loads[1 + part].wait()

            def store(i, h, x):
                new_t[h, part, i * 16:(i + 1) * 16, :] = x
            head_major(lambda i: block[i], wide, store, block.shape[0])
        loads[3].wait()

    for t in range(N_CH + LAG):
        if t < N_CH:
            z_wait(t, zr_sem)
            step1(t)
        if t == 0:
            new_keys()
        if 1 <= t <= N_CH:
            step2(t - 1)
        if t == 2:
            fits_vec[...] = jnp.broadcast_to(capacity_check(table, named_by_column), fits_vec.shape)
            fits_copy.start()
        if t >= LAG:
            attend(t - LAG)
    fits_copy.wait()
    for ch in range(N_CH):
        z_wait(ch, zs_sem)
    for i in range(2 * N_CH):
        wait1(i, s1_sem)
        wait2(i, s2_sem)


def exchange_attention(table_t, q, zsend, k_new, v_new, per_dev):
    tokens, dim = zsend.shape[3:]
    dtype = q.dtype
    hbm = pl.BlockSpec(memory_space=pl.ANY)
    recv = pltpu.VMEM((N_CH, RING, RING, 2, PAIR_CAP * tokens, dim), dtype)
    tables = [(2 * RING, 128), (2 * RING * PAIR_CAP, table_t.shape[1])]
    return pl.pallas_call(
        functools.partial(exchange_kernel, per_dev),
        out_shape=[pltpu.VMEM(q.shape, dtype), jax.ShapeDtypeStruct((8, 128), jnp.int32)],
        in_specs=[hbm] * 5,
        out_specs=[pl.BlockSpec(memory_space=pltpu.VMEM), hbm],
        scratch_shapes=[pltpu.VMEM(q.shape, dtype), recv, recv,
                        pltpu.VMEM(k_new.shape, dtype), pltpu.VMEM(v_new.shape, dtype), pltpu.VMEM((N_CH, 2, q.shape[0], q.shape[2]), dtype),
                        pltpu.VMEM((4,) + k_new.shape[1:], jnp.float32), pltpu.VMEM(zsend.shape, dtype), pltpu.VMEM(table_t.shape, jnp.int32)]
        + [pltpu.VMEM(shape, jnp.int32) for shape in tables] + [pltpu.SMEM(shape, jnp.int32) for shape in tables]
        + [pltpu.VMEM((PLANE, 128), jnp.float32), pltpu.VMEM((8, 128), jnp.int32)]
        + [pltpu.VMEM((PLANES * Z_CAP, 2, tokens, dim), dtype)] * N_CH
        + [pltpu.VMEM((RING, GROUP_CAP, tokens, dim), dtype)] * (2 * N_CH)
        + [pltpu.VMEM((RING * GROUP_CAP, tokens, dim), dtype)] * (2 * N_CH)
        + [pltpu.VMEM((2 * RING, RING, PAIR_CAP * tokens, dim), dtype)] * (2 * N_CH)
        + [pltpu.SemaphoreType.DMA((N_CH,))] * 2 + [pltpu.SemaphoreType.DMA((2 * N_CH,))] * 4 + [pltpu.SemaphoreType.DMA((N_CH,))],
        compiler_params=pltpu.CompilerParams(collective_id=0, has_side_effects=True, vmem_limit_bytes=48 << 20),
        name='exchange_attention',
    )(table_t, q, zsend, k_new, v_new)


def attention_kernel(q_ref, kv_ref, new_ref, out_ref):
    head_dim = q_ref.shape[2]
    attend_head(q_ref, lambda part: kv_ref[0, :, part].reshape(-1, head_dim), lambda part: new_ref[0, part], out_ref, 0)


def attention(q, kv, new):
    chunk_len, q_heads, head_dim = q.shape
    return pl.pallas_call(
        attention_kernel,
        grid=(N_CH,),
        out_shape=jax.ShapeDtypeStruct(q.shape, q.dtype),
        in_specs=[pl.BlockSpec((chunk_len, GROUP, head_dim), lambda c: (0, c, 0)),
                  pl.BlockSpec((1,) + kv.shape[1:], lambda c: (c, 0, 0, 0, 0)),
                  pl.BlockSpec((1,) + new.shape[1:], lambda c: (c, 0, 0, 0))],
        out_specs=pl.BlockSpec((chunk_len, GROUP, head_dim), lambda c: (0, c, 0)),
        compiler_params=pltpu.CompilerParams(vmem_limit_bytes=48 << 20),
        name='attention',
    )(q, kv, new)


def by_chunk(k, v):
    n, t, h, d = k.shape
    both = jnp.stack([k, v], axis=1).reshape(n, 2, t, N_CH, h // N_CH, d)
    return both.transpose(0, 3, 1, 4, 2, 5).reshape(n, N_CH, 2 * h // N_CH, t, d)


def solution(mesh):
    n_dev = mesh.shape['pool']

    def padded_exchange(k_pool, v_pool, block_table):
        per_dev = k_pool.shape[0]
        n_pref = block_table.shape[1]
        my_index = lax.axis_index('pool')
        pair_cap = 2
        owners = block_table // per_dev
        owned_here = (owners == my_index).astype(jnp.int32)
        send_slot = jnp.where(owned_here > 0, jnp.cumsum(owned_here, axis=1) - 1, pair_cap)
        dest_dev = jnp.broadcast_to(jnp.arange(n_dev)[:, None], send_slot.shape)
        send_ids = jnp.zeros((n_dev, pair_cap), jnp.int32).at[dest_dev, send_slot].set(block_table % per_dev, mode='drop')
        k_recv = lax.all_to_all(k_pool[send_ids], 'pool', 0, 0, tiled=True)
        v_recv = lax.all_to_all(v_pool[send_ids], 'pool', 0, 0, tiled=True)
        my_owners = lax.dynamic_slice_in_dim(owners, my_index, 1, 0).reshape(-1)
        from_owner = (my_owners[:, None] == jnp.arange(n_dev)[None, :]).astype(jnp.int32)
        slot_rank = jnp.sum(from_owner * (jnp.cumsum(from_owner, axis=0) - 1), axis=1)
        recv_idx = my_owners * pair_cap + slot_rank
        flat = (n_dev * pair_cap,) + k_pool.shape[1:]
        pairs = by_chunk(k_recv.reshape(flat)[recv_idx], v_recv.reshape(flat)[recv_idx])
        parts, t, d = pairs.shape[2:]
        pairs = pairs.reshape(n_pref // PAIR_CAP, PAIR_CAP, N_CH, parts, t, d).transpose(2, 0, 3, 1, 4, 5)
        return pairs.reshape(N_CH, n_pref // PAIR_CAP, parts, PAIR_CAP * t, d)

    def local_step(queries, k_new, v_new, k_pool, v_pool, block_table, write_ids):
        block_len = k_pool.shape[1]
        new_shape = (queries.shape[1] // block_len, block_len) + k_new.shape[2:]
        k_blocks, v_blocks = k_new.reshape(new_shape), v_new.reshape(new_shape)
        k_pool_out, v_pool_out, zsend = prepare(write_ids, block_table.T, k_pool, v_pool, k_blocks, v_blocks)
        fast, fits = exchange_attention(block_table.T, queries[0], zsend, k_blocks, v_blocks, k_pool.shape[0])
        attn_out = lax.cond(
            fits[0, 0] > 0,
            lambda: fast,
            lambda: attention(queries[0], padded_exchange(k_pool, v_pool, block_table), by_chunk(k_new, v_new)[0]))[None]
        return attn_out, k_pool_out, v_pool_out

    row_spec = P('pool')
    return jax.shard_map(local_step, mesh=mesh, in_specs=(row_spec, row_spec, row_spec, row_spec, row_spec, P(), row_spec), out_specs=(row_spec, row_spec, row_spec), check_vma=False)
```

```python
import functools

import jax
import jax.numpy as jnp
from jax import lax
from jax.experimental import pallas as pl
from jax.experimental.pallas import tpu as pltpu
from jax.sharding import PartitionSpec as P

MESH = pl.DeviceIdType.MESH
PLANES = 4
PLANE = 32
Z_CAP = 10
PAIR_CAP = 2
N_CH = 8
GROUP = 8
TILE = 32
LOG2E = 1.4426950408889634
RING = 4
GROUP_CAP = 10
LAG = 3
STEPS = (1, 3, 2)


def attend_head(q_ref, kv, new, out_ref, ch):
    chunk_len, head_dim = q_ref.shape[0], q_ref.shape[2]
    scale = head_dim ** -0.5 * LOG2E
    heads = pl.ds(ch * GROUP, GROUP)
    k_pref, v_pref = kv(0), kv(1)
    k_new, v_new = new(0), new(1)

    def scores(t):
        q = q_ref[pl.ds(t * TILE, TILE), heads, :].astype(jnp.float32).reshape(TILE * GROUP, head_dim).astype(jnp.bfloat16)
        return nt(q, k_pref), nt(q, k_new)

    n_tile = chunk_len // TILE
    ahead = scores(0)
    for t in range(n_tile):
        s_pref, s_self = ahead
        if t + 1 < n_tile:
            ahead = scores(t + 1)
        token = t * TILE + lax.broadcasted_iota(jnp.int32, s_self.shape, 0) // GROUP
        s_self = jnp.where(token >= lax.broadcasted_iota(jnp.int32, s_self.shape, 1), s_self, -jnp.inf)
        top = jnp.maximum(jnp.max(s_pref, axis=1, keepdims=True), jnp.max(s_self, axis=1, keepdims=True))
        e_pref = jnp.exp2((s_pref - top) * scale)
        e_self = jnp.exp2((s_self - top) * scale)
        inv = 1.0 / (jnp.sum(e_pref, axis=1, keepdims=True) + jnp.sum(e_self, axis=1, keepdims=True))
        p_pref = (e_pref * inv).astype(jnp.bfloat16)
        p_self = (e_self * inv).astype(jnp.bfloat16)
        acc = jnp.dot(p_pref, v_pref, preferred_element_type=jnp.float32) + jnp.dot(p_self, v_new, preferred_element_type=jnp.float32)
        out_ref[pl.ds(t * TILE, TILE), heads, :] = acc.reshape(TILE, GROUP, head_dim).astype(jnp.bfloat16)


def head_major(src, wide, store, blocks):
    for i in range(blocks):
        tokens, heads, dim = wide.shape[1:]
        slot = i % wide.shape[0]
        wide[slot] = src(i).astype(jnp.float32)
        flat = wide.at[slot].reshape(tokens * heads, dim)
        for h in range(heads):
            store(i, h, flat[pl.ds(h, tokens, stride=heads), :].astype(jnp.bfloat16))


def iota(shape, dim):
    return lax.broadcasted_iota(jnp.int32, shape, dim)


def flag(mask):
    return jnp.where(mask, 1.0, 0.0).astype(jnp.bfloat16)


def nt(a, b):
    return lax.dot_general(a, b, (((1,), (1,)), ((), ())), preferred_element_type=jnp.float32)


class Table:
    def __init__(self, table, per_dev):
        owner = table // per_dev
        self.per_dev, self.n_key, self.n_row = per_dev, PLANES * per_dev, table.shape[1]
        self.col = owner % PLANE
        self.key = owner // PLANE * per_dev + table % per_dev

    def hots(self, q):
        match = self.col == q
        ends = (jnp.min(jnp.where(match, self.key, self.n_key - 1), axis=0, keepdims=True), jnp.max(jnp.where(match, self.key, 0), axis=0, keepdims=True))
        return [flag(iota((self.n_key, self.n_row), 0) == end) for end in ends]

    def slots(self, q):
        first, last = self.hots(q)
        every = flag(iota((8, self.n_row), 0) >= 0)
        named = jnp.where(nt(every, first) + nt(every, last) > 0, 1.0, 0.0)
        i, j = iota((self.n_key, self.n_key), 0), iota((self.n_key, self.n_key), 1)
        before = flag((i < j) & (i // self.per_dev == j // self.per_dev))
        rank = jnp.dot(named.astype(jnp.bfloat16), before, preferred_element_type=jnp.float32)
        return named[:1], rank[:1]


def prepare_kernel(wid_hbm, table_hbm, k_pool_hbm, v_pool_hbm, k_new_hbm, v_new_hbm, k_out_hbm, v_out_hbm, zsend_ref,
                   table_ref, k_pool, v_pool, k_new, v_new, idx_vec, idx_smem, wid_ref, wide, in_sem, out_sem, idx_sem, wid_sem):
    me = lax.axis_index('pool')
    my_z, my_pos = me // PLANE, lax.rem(me, PLANE)
    per_dev = k_pool.shape[0]
    get_table = pltpu.make_async_copy(table_hbm, table_ref, idx_sem)
    get_table.start()
    get_ids = pltpu.make_async_copy(wid_hbm, wid_ref, wid_sem)
    get_ids.start()
    loads = [pltpu.make_async_copy(src, dst, in_sem.at[i]) for i, (src, dst) in enumerate(
        ((k_pool_hbm, k_pool), (v_pool_hbm, v_pool), (k_new_hbm, k_new), (v_new_hbm, v_new)))]
    for copy in loads:
        copy.start()
    get_table.wait()
    table = Table(table_ref[...], per_dev)
    named, rank = table.slots(my_pos)
    key = iota((16, table.n_key), 1)
    hit = (named > 0) & (rank == iota((16, table.n_key), 0).astype(jnp.float32)) & (key // per_dev == my_z)
    chosen = jnp.sum(jnp.where(hit, key % per_dev, 0), axis=1, keepdims=True)
    idx_vec[...] = jnp.broadcast_to(chosen, idx_vec.shape)
    to_smem = pltpu.make_async_copy(idx_vec, idx_smem, idx_sem)
    to_smem.start()

    for copy in loads:
        copy.wait()
    pools = [pltpu.make_async_copy(src, dst, out_sem.at[i]) for i, (src, dst) in enumerate(((k_pool, k_out_hbm), (v_pool, v_out_hbm)))]
    for copy in pools:
        copy.start()
    to_smem.wait()
    get_ids.wait()

    def send_blocks(part, pool):
        def store(i, h, x):
            zsend_ref[h, i, part] = x
        head_major(lambda i: pool[idx_smem[i, 0]], wide, store, Z_CAP)

    send_blocks(0, k_pool)
    for copy in pools:
        copy.wait()
    writes = []
    for i in range(k_new.shape[0]):
        for part, (src, dst) in enumerate(((k_new, k_out_hbm), (v_new, v_out_hbm))):
            writes.append(pltpu.make_async_copy(src.at[i], dst.at[wid_ref[0, i]], in_sem.at[2 * i + part]))
            writes[-1].start()
    send_blocks(1, v_pool)
    for copy in writes:
        copy.wait()


def prepare(write_ids, table_t, k_pool, v_pool, k_new, v_new):
    tokens, heads, dim = k_pool.shape[1:]
    vmem, hbm = (pl.BlockSpec(memory_space=m) for m in (pltpu.VMEM, pl.ANY))
    return pl.pallas_call(
        prepare_kernel,
        out_shape=[jax.ShapeDtypeStruct(k_pool.shape, k_pool.dtype), jax.ShapeDtypeStruct(v_pool.shape, v_pool.dtype),
                   jax.ShapeDtypeStruct((N_CH, Z_CAP, 2, tokens, dim), k_pool.dtype)],
        in_specs=[pl.BlockSpec(memory_space=pltpu.HBM)] + [hbm] * 5,
        out_specs=[hbm, hbm, vmem],
        scratch_shapes=[pltpu.VMEM(table_t.shape, jnp.int32), pltpu.VMEM(k_pool.shape, k_pool.dtype), pltpu.VMEM(k_pool.shape, k_pool.dtype),
                        pltpu.VMEM(k_new.shape, k_pool.dtype), pltpu.VMEM(k_new.shape, k_pool.dtype),
                        pltpu.VMEM((16, 128), jnp.int32), pltpu.SMEM((16, 128), jnp.int32), pltpu.SMEM(write_ids.shape, jnp.int32),
                        pltpu.VMEM((4, tokens, heads, dim), jnp.float32),
                        pltpu.SemaphoreType.DMA((2 * k_new.shape[0],)), pltpu.SemaphoreType.DMA((2,)), pltpu.SemaphoreType.DMA, pltpu.SemaphoreType.DMA],
        compiler_params=pltpu.CompilerParams(vmem_limit_bytes=32 << 20),
        name='prepare',
    )(write_ids, table_t, k_pool, v_pool, k_new, v_new)


def members(n_group, n_row, plane_of):
    group, row = iota((n_group, n_row), 0), iota((n_group, n_row), 1)
    at = jnp.where(group // RING % 2 == 0, row // 8 % RING, row // 2 % RING)
    return flag((row // PLANE == plane_of(group)) & (at == group % RING))


def capacity_check(table, named_by_column):
    groups = members(2 * RING * PLANES, table.n_row, lambda g: g // (2 * RING))
    n_group = groups.shape[0]

    def widest(q, most):
        first, last = table.hots(q)
        named = jnp.where(nt(groups, first) + nt(groups, last) > 0, 1.0, 0.0)
        named_by_column[pl.ds(q, 1), :] = jnp.max(named, axis=0, keepdims=True)
        return jnp.maximum(most, jnp.sum(named, axis=1, keepdims=True))

    most_in_group = lax.fori_loop(0, PLANE, widest, jnp.zeros((n_group, 1), jnp.float32), unroll=4)
    per_plane = flag(iota((table.n_key, 128), 0) // table.per_dev == iota((table.n_key, 128), 1))
    by_device = jnp.dot(named_by_column[...].astype(jnp.bfloat16), per_plane, preferred_element_type=jnp.float32)
    in_col = jnp.zeros((1, table.n_row), jnp.int32)
    for q in range(PLANE):
        in_col = jnp.maximum(in_col, jnp.sum(jnp.where(table.col == q, 1, 0), axis=0, keepdims=True))

    def top(a):
        return jnp.max(jnp.max(a, axis=1, keepdims=True), axis=0, keepdims=True)

    return jnp.where((top(in_col) <= PAIR_CAP) & (top(by_device) <= Z_CAP) & (top(most_in_group) <= GROUP_CAP), 1, 0)


def routing(table, my_z, my_y, my_x, my_c, first_ref, second_ref):
    n_key, n_row = table.n_key, table.n_row
    my_pos = my_y * 8 + my_x * 2 + my_c
    _, rank = table.slots(my_pos)
    slot_row = jnp.minimum(rank, Z_CAP - 1.0) + (iota(rank.shape, 1) // table.per_dev * Z_CAP).astype(jnp.float32)
    groups = members(2 * RING, n_row, lambda g: my_z)
    before = flag(iota((n_key, n_key), 0) < iota((n_key, n_key), 1))

    def lists(q):
        hots = table.hots(q)
        listed = jnp.where(nt(groups, hots[0]) + nt(groups, hots[1]) > 0, 1.0, 0.0)
        return hots, listed, jnp.dot(listed.astype(jnp.bfloat16), before, preferred_element_type=jnp.float32)

    _, listed, place = lists(my_pos)
    first_step = jnp.zeros((2 * RING, 128), jnp.int32)
    for i in range(GROUP_CAP):
        at = jnp.sum(jnp.where((listed > 0) & (place == i), slot_row, 0.0), axis=1, keepdims=True).astype(jnp.int32)
        first_step = jnp.where(iota(first_step.shape, 1) == i, at, first_step)
    first_ref[...] = jnp.clip(first_step, 0, PLANES * Z_CAP - 1)
    for part in range(2):
        for src in range(RING):
            q = (src * 8 + my_x * 2 + my_c) if part == 0 else (my_y * 8 + src * 2 + my_c)
            mine_at = my_y if part == 0 else RING + my_x
            hots, _, place = lists(q)
            for end in range(PAIR_CAP):
                found = jnp.dot(place.astype(jnp.bfloat16), hots[end], preferred_element_type=jnp.float32)
                found = jnp.sum(jnp.where(iota(found.shape, 0) == mine_at, found, 0.0), axis=0, keepdims=True)
                line = (part * RING + src) * PAIR_CAP + end
                second_ref[line:line + 1, :] = jnp.clip(found.astype(jnp.int32), 0, GROUP_CAP - 1) + src * GROUP_CAP


def exchange_kernel(per_dev, table_hbm, q_hbm, zsend_hbm, k_new_hbm, v_new_hbm, out_ref, fits_hbm, q_ref, recv_k, recv_v, k_new, v_new,
                    new_t, wide, zsend, table_ref, first_vec, second_vec, first_ref, second_ref, named_by_column, fits_vec, *scratch):
    zrecv, send1, recv1, send2 = (scratch[:N_CH], scratch[N_CH:3 * N_CH], scratch[3 * N_CH:5 * N_CH], scratch[5 * N_CH:7 * N_CH])
    zs_sem, zr_sem, s1_sem, r1_sem, s2_sem, r2_sem, in_sem = scratch[7 * N_CH:]
    me = lax.axis_index('pool')
    my_z, my_pos = me // PLANE, lax.rem(me, PLANE)
    base = my_z * PLANE
    y, x, c = my_pos // 8, lax.rem(my_pos // 2, RING), lax.rem(my_pos, 2)
    head_dim = q_ref.shape[2]

    def z_peer(d):
        return lax.rem(my_z + d, PLANES) * PLANE + my_pos

    def y_peer(d, dc):
        return base + lax.rem(y + d, RING) * 8 + x * 2 + lax.rem(c + dc, 2)

    def x_peer(d, dc):
        return base + y * 8 + lax.rem(x + d, RING) * 2 + lax.rem(c + dc, 2)

    barrier = pltpu.get_barrier_semaphore()
    peers = [z_peer(d) for d in STEPS] + [peer(d, dc) for d in STEPS for dc in range(2) for peer in (y_peer, x_peer)] + [y_peer(0, 1)]
    for peer in peers:
        pl.semaphore_signal(barrier, inc=1, device_id=(peer,), device_id_type=MESH)

    loads = [pltpu.make_async_copy(src, dst, in_sem.at[i]) for i, (src, dst) in enumerate(
        ((zsend_hbm, zsend), (k_new_hbm, k_new), (v_new_hbm, v_new), (q_hbm, q_ref), (table_hbm, table_ref)))]
    to_smem = [pltpu.make_async_copy(src, dst, in_sem.at[5 + i]) for i, (src, dst) in enumerate(((first_vec, first_ref), (second_vec, second_ref)))]
    fits_copy = pltpu.make_async_copy(fits_vec, fits_hbm, in_sem.at[7])
    for copy in loads:
        copy.start()

    def remote(src, dst, send_sem, recv_sem, peer):
        return pltpu.make_async_remote_copy(
            src_ref=src, dst_ref=dst, send_sem=send_sem, recv_sem=recv_sem, device_id=(peer,), device_id_type=MESH)

    def wait_bytes(ref, sem):
        pltpu.make_async_copy(ref, ref, sem).wait()

    def z_wait(ch, sem):
        wait_bytes(zrecv[ch].at[pl.ds(0, (PLANES - 1) * Z_CAP)], sem.at[ch])

    def wait1(i, sem):
        wait_bytes(recv1[i].at[pl.ds(0, (RING - 1) * GROUP_CAP)], sem.at[i])

    def wait2(i, sem):
        wait_bytes(send2[i].at[pl.ds(0, 2 * RING - 1)], sem.at[i])

    def step1(ch):
        for part in range(2):
            i = 2 * ch + part
            for g in range(RING):
                for s in range(GROUP_CAP):
                    send1[i][g, s] = zrecv[ch][first_ref[part * RING + g, s], part]
            mine = y if part == 0 else x
            recv1[i][pl.ds(mine * GROUP_CAP, GROUP_CAP)] = send1[i][mine]
        for d in STEPS:
            for part in range(2):
                i = 2 * ch + part
                mine, peer = (y, y_peer(d, 0)) if part == 0 else (x, x_peer(d, 0))
                remote(send1[i].at[lax.rem(mine + d, RING)], recv1[i].at[pl.ds(mine * GROUP_CAP, GROUP_CAP)],
                       s1_sem.at[i], r1_sem.at[i], peer).start()

    def step2(ch):
        for part in range(2):
            i = 2 * ch + part
            wait1(i, r1_sem)

            @pl.loop(0, RING)
            def _(to):
                for core in range(2):
                    row = base + ((y * 8 + to * 2) if part == 0 else (to * 8 + x * 2)) + core
                    for src in range(RING):
                        for end in range(PAIR_CAP):
                            send2[i][to * 2 + core, src, end * 16:(end + 1) * 16, :] = recv1[i][second_ref[(part * RING + src) * PAIR_CAP + end, row]]

        recv_k[ch, :, x, c] = send2[2 * ch][x * 2 + c]
        recv_v[ch, y, :, c] = send2[2 * ch + 1][y * 2 + c]
        for d in STEPS + (0,):
            for dc in range(2):
                for part in range(2):
                    if (d, dc) == (0, 0):
                        continue
                    i = 2 * ch + part
                    mine, peer = (x, x_peer(d, dc)) if part == 0 else (y, y_peer(d, dc))
                    dst = recv_k.at[ch, :, x, c] if part == 0 else recv_v.at[ch, y, :, c]
                    remote(send2[i].at[lax.rem(mine + d, RING) * 2 + lax.rem(c + dc, 2)], dst, s2_sem.at[i], r2_sem.at[i], peer).start()

    def attend(ch):
        wait2(2 * ch, r2_sem)
        wait2(2 * ch + 1, r2_sem)
        recv = (recv_k, recv_v)
        attend_head(q_ref, lambda part: recv[part][ch].reshape(-1, head_dim), lambda part: new_t[ch, part], out_ref, ch)

    loads[0].wait()
    pl.semaphore_wait(barrier, len(peers))
    for ch in range(N_CH):
        for d in STEPS:
            remote(zsend.at[ch], zrecv[ch].at[pl.ds(my_z * Z_CAP, Z_CAP)], zs_sem.at[ch], zr_sem.at[ch], z_peer(d)).start()
    loads[4].wait()
    table = Table(table_ref[...], per_dev)
    routing(table, my_z, y, x, c, first_vec, second_vec)
    for copy in to_smem:
        copy.start()
    for ch in range(N_CH):
        zrecv[ch][pl.ds(my_z * Z_CAP, Z_CAP)] = zsend[ch]
    for copy in to_smem:
        copy.wait()

    def new_keys():
        for part, block in enumerate((k_new, v_new)):
            loads[1 + part].wait()

            def store(i, h, x):
                new_t[h, part, i * 16:(i + 1) * 16, :] = x
            head_major(lambda i: block[i], wide, store, block.shape[0])
        loads[3].wait()

    for t in range(N_CH + LAG):
        if t < N_CH:
            z_wait(t, zr_sem)
            step1(t)
        if t == 0:
            new_keys()
        if 1 <= t <= N_CH:
            step2(t - 1)
        if t == 2:
            fits_vec[...] = jnp.broadcast_to(capacity_check(table, named_by_column), fits_vec.shape)
            fits_copy.start()
        if t >= LAG:
            attend(t - LAG)
    fits_copy.wait()
    for ch in range(N_CH):
        z_wait(ch, zs_sem)
    for i in range(2 * N_CH):
        wait1(i, s1_sem)
        wait2(i, s2_sem)


def exchange_attention(table_t, q, zsend, k_new, v_new, per_dev):
    tokens, dim = zsend.shape[3:]
    dtype = q.dtype
    hbm = pl.BlockSpec(memory_space=pl.ANY)
    recv = pltpu.VMEM((N_CH, RING, RING, 2, PAIR_CAP * tokens, dim), dtype)
    tables = [(2 * RING, 128), (2 * RING * PAIR_CAP, table_t.shape[1])]
    return pl.pallas_call(
        functools.partial(exchange_kernel, per_dev),
        out_shape=[pltpu.VMEM(q.shape, dtype), jax.ShapeDtypeStruct((8, 128), jnp.int32)],
        in_specs=[hbm] * 5,
        out_specs=[pl.BlockSpec(memory_space=pltpu.VMEM), hbm],
        scratch_shapes=[pltpu.VMEM(q.shape, dtype), recv, recv,
                        pltpu.VMEM(k_new.shape, dtype), pltpu.VMEM(v_new.shape, dtype), pltpu.VMEM((N_CH, 2, q.shape[0], q.shape[2]), dtype),
                        pltpu.VMEM((4,) + k_new.shape[1:], jnp.float32), pltpu.VMEM(zsend.shape, dtype), pltpu.VMEM(table_t.shape, jnp.int32)]
        + [pltpu.VMEM(shape, jnp.int32) for shape in tables] + [pltpu.SMEM(shape, jnp.int32) for shape in tables]
        + [pltpu.VMEM((PLANE, 128), jnp.float32), pltpu.VMEM((8, 128), jnp.int32)]
        + [pltpu.VMEM((PLANES * Z_CAP, 2, tokens, dim), dtype)] * N_CH
        + [pltpu.VMEM((RING, GROUP_CAP, tokens, dim), dtype)] * (2 * N_CH)
        + [pltpu.VMEM((RING * GROUP_CAP, tokens, dim), dtype)] * (2 * N_CH)
        + [pltpu.VMEM((2 * RING, RING, PAIR_CAP * tokens, dim), dtype)] * (2 * N_CH)
        + [pltpu.SemaphoreType.DMA((N_CH,))] * 2 + [pltpu.SemaphoreType.DMA((2 * N_CH,))] * 4 + [pltpu.SemaphoreType.DMA((N_CH,))],
        compiler_params=pltpu.CompilerParams(collective_id=0, has_side_effects=True, vmem_limit_bytes=48 << 20),
        name='exchange_attention',
    )(table_t, q, zsend, k_new, v_new)


def attention_kernel(q_ref, kv_ref, new_ref, out_ref):
    head_dim = q_ref.shape[2]
    attend_head(q_ref, lambda part: kv_ref[0, :, part].reshape(-1, head_dim), lambda part: new_ref[0, part], out_ref, 0)


def attention(q, kv, new):
    chunk_len, q_heads, head_dim = q.shape
    return pl.pallas_call(
        attention_kernel,
        grid=(N_CH,),
        out_shape=jax.ShapeDtypeStruct(q.shape, q.dtype),
        in_specs=[pl.BlockSpec((chunk_len, GROUP, head_dim), lambda c: (0, c, 0)),
                  pl.BlockSpec((1,) + kv.shape[1:], lambda c: (c, 0, 0, 0, 0)),
                  pl.BlockSpec((1,) + new.shape[1:], lambda c: (c, 0, 0, 0))],
        out_specs=pl.BlockSpec((chunk_len, GROUP, head_dim), lambda c: (0, c, 0)),
        compiler_params=pltpu.CompilerParams(vmem_limit_bytes=48 << 20),
        name='attention',
    )(q, kv, new)


def by_chunk(k, v):
    n, t, h, d = k.shape
    both = jnp.stack([k, v], axis=1).reshape(n, 2, t, N_CH, h // N_CH, d)
    return both.transpose(0, 3, 1, 4, 2, 5).reshape(n, N_CH, 2 * h // N_CH, t, d)


def solution(mesh):
    n_dev = mesh.shape['pool']

    def padded_exchange(k_pool, v_pool, block_table):
        per_dev = k_pool.shape[0]
        n_pref = block_table.shape[1]
        my_index = lax.axis_index('pool')
        pair_cap = 2
        owners = block_table // per_dev
        owned_here = (owners == my_index).astype(jnp.int32)
        send_slot = jnp.where(owned_here > 0, jnp.cumsum(owned_here, axis=1) - 1, pair_cap)
        dest_dev = jnp.broadcast_to(jnp.arange(n_dev)[:, None], send_slot.shape)
        send_ids = jnp.zeros((n_dev, pair_cap), jnp.int32).at[dest_dev, send_slot].set(block_table % per_dev, mode='drop')
        k_recv = lax.all_to_all(k_pool[send_ids], 'pool', 0, 0, tiled=True)
        v_recv = lax.all_to_all(v_pool[send_ids], 'pool', 0, 0, tiled=True)
        my_owners = lax.dynamic_slice_in_dim(owners, my_index, 1, 0).reshape(-1)
        from_owner = (my_owners[:, None] == jnp.arange(n_dev)[None, :]).astype(jnp.int32)
        slot_rank = jnp.sum(from_owner * (jnp.cumsum(from_owner, axis=0) - 1), axis=1)
        recv_idx = my_owners * pair_cap + slot_rank
        flat = (n_dev * pair_cap,) + k_pool.shape[1:]
        pairs = by_chunk(k_recv.reshape(flat)[recv_idx], v_recv.reshape(flat)[recv_idx])
        parts, t, d = pairs.shape[2:]
        pairs = pairs.reshape(n_pref // PAIR_CAP, PAIR_CAP, N_CH, parts, t, d).transpose(2, 0, 3, 1, 4, 5)
        return pairs.reshape(N_CH, n_pref // PAIR_CAP, parts, PAIR_CAP * t, d)

    def local_step(queries, k_new, v_new, k_pool, v_pool, block_table, write_ids):
        block_len = k_pool.shape[1]
        new_shape = (queries.shape[1] // block_len, block_len) + k_new.shape[2:]
        k_blocks, v_blocks = k_new.reshape(new_shape), v_new.reshape(new_shape)
        k_pool_out, v_pool_out, zsend = prepare(write_ids, block_table.T, k_pool, v_pool, k_blocks, v_blocks)
        fast, fits = exchange_attention(block_table.T, queries[0], zsend, k_blocks, v_blocks, k_pool.shape[0])
        attn_out = lax.cond(
            fits[0, 0] > 0,
            lambda: fast,
            lambda: attention(queries[0], padded_exchange(k_pool, v_pool, block_table), by_chunk(k_new, v_new)[0]))[None]
        return attn_out, k_pool_out, v_pool_out

    row_spec = P('pool')
    return jax.shard_map(local_step, mesh=mesh, in_specs=(row_spec, row_spec, row_spec, row_spec, row_spec, P(), row_spec), out_specs=(row_spec, row_spec, row_spec), check_vma=False)
```
